128 devices in a mesh: ctx: 16 (over x, z), head: 8 (over y, core).
Axes of the slice: x: 4, y: 4, z: 4, core: 2. Of those that a mesh axis runs over, the one named last changes fastest.
Arguments:
- input_x_channels: bfloat16 [16384, 8192], P('ctx', 'head'), may hold values from -4 to 4
- input_b_channels: bfloat16 [16384, 1024], P('ctx', 'head'), may hold values from -3 to 3
- input_c_channels: bfloat16 [16384, 1024], P('ctx', 'head'), may hold values from -3 to 3
- input_gate_channels: bfloat16 [16384, 8192], P('ctx', 'head'), may hold values from -75 to 75
- raw_step_sizes: float32 [128, 16384], P('head', 'ctx'), may hold values from -7 to 800
- log_decay_rate: float32 [128], P('head'), may hold values from -8 to -2.3
- head_skip_coeff: float32 [128], P('head'), may hold values from 0.5 to 2
- x_conv_taps: bfloat16 [4, 8192], P(None, 'head'), may hold values from -3 to 3
- b_conv_taps: bfloat16 [4, 1024], P(None, 'head'), may hold values from -3 to 3
- c_conv_taps: bfloat16 [4, 1024], P(None, 'head'), may hold values from -3 to 3
- gated_norm_gain: bfloat16 [8192], P('head'), may hold values from 0.099609375 to 1.8984375
- output_weight: bfloat16 [8192, 4096], P('head'), may hold values from -0.0625 to 0.0625
- adapter_down_panels: bfloat16 [96, 8192, 64], P('ctx', 'head'), may hold values from -0.0625 to 0.0625
- adapter_up_panels: bfloat16 [96, 64, 4096], P('ctx', None, 'head'), may hold values from -0.75 to 0.75
- turn_first_token: int32 [32], replicated, may hold values from 0 to 16256, as said below
- tenant_of_turn: int32 [32], replicated, may hold values from 0 to 95
- tenant_panel_index: int32 [96], replicated, may hold values from 0 to 95, each once
Outputs:
- out: bfloat16 [16384, 4096], P('ctx', 'head')
The draws below stay inside these ranges and needn't reach their ends.
Inputs may be any that keep to these rules, and one draw needn't show every extreme that they name: `turn_first_token`: strictly increasing multiples of 128; the first is 0; every aligned block of 1024 tokens holds exactly 2 starts, and in every block but the first the earlier of them lies past the block's first token.
All inputs are finite; a program needn't handle non-finite values.
Results may differ from the reference program's by a relative error of at most 0.014.
Values may be sent and summed in bfloat16 or wider, within the bound.
A program may use at most 128 MiB of HBM per device.

```python
import math
import jax
import jax.numpy as jnp
import numpy as np
from jax import lax

MODEL_WIDTH = 4096
H = 128
P_SIZE = 64
N = 128
G = 8
K = 4
Q = 128
ADAPTER_RANK = 64
UNIT = 128
TOK_DEV = 1024
TOKENS = 16384
INNER_CHANNELS = 8192
GN = 1024
TENANT_COUNT = 96
TURNS = 32


def head_plan(key):
    picks = jax.random.randint(jax.random.fold_in(key, 101), (H,), 0, 8)
    quick_heads = picks < 4
    uniform_draw = jax.random.uniform(jax.random.fold_in(key, 102), (H,), jnp.float32)
    quick_rate = jnp.exp(math.log(0.03) + uniform_draw * math.log(0.1 / 0.03))
    patient_rate = (0.4 + 0.4 * uniform_draw) / (3.0 * math.sqrt(TOKENS))
    decay_rate = jnp.where(quick_heads, quick_rate, patient_rate)
    spot_places = jax.random.randint(jax.random.fold_in(key, 104), (3,), 0, TOKENS)
    strength = 0.22 + 0.23 * jax.random.uniform(jax.random.fold_in(key, 105), (3, H), jnp.float32)
    surge_steps = strength / decay_rate[None, :]
    return (quick_heads, decay_rate, spot_places, surge_steps)


def draw_log_decay_rate(key, part):
    quick_heads, decay_rate, spot_places, surge_steps = head_plan(key)
    return jnp.log(decay_rate)


def draw_raw_step_sizes(key, part):
    quick_heads, decay_rate, spot_places, surge_steps = head_plan(key)
    uniform_draw = jax.random.uniform(jax.random.fold_in(key, 103), (H, TOKENS), jnp.float32)
    slow_scale = 3.0 / math.sqrt(TOKENS)
    quick_steps = 0.4 + 0.9 * uniform_draw
    slow_steps = slow_scale * (0.5 + uniform_draw)
    step_sizes = jnp.where(quick_heads[:, None], quick_steps, slow_steps)
    places = jnp.arange(TOKENS)
    for which in range(3):
        at_spot = places == spot_places[which]
        step_sizes = jnp.where(at_spot[None, :], surge_steps[which][:, None], step_sizes)
    return step_sizes + jnp.log(-jnp.expm1(-step_sizes))


def draw_input_x_channels(key, part):
    quick_heads, decay_rate, spot_places, surge_steps = head_plan(key)
    noise_key = jax.random.fold_in(key, 106)
    noise_draw = jax.random.truncated_normal(noise_key, -4.0, 4.0, (TOKENS, H, P_SIZE), jnp.float32)
    places = jnp.arange(TOKENS)
    factor = jnp.ones((TOKENS, H), jnp.float32)
    for which in range(3):
        near_spot = (places >= spot_places[which] - (K - 1)) & (places <= spot_places[which])
        factor = factor * jnp.where(near_spot[:, None], 1.0 / surge_steps[which][None, :], 1.0)
    return (noise_draw * factor[:, :, None]).reshape(TOKENS, H * P_SIZE).astype(jnp.bfloat16)


def draw_input_gate_channels(key, part):
    noise_key = jax.random.fold_in(key, 301)
    row_key = jax.random.fold_in(key, 302)
    column_key = jax.random.fold_in(key, 303)
    noise_draw = jax.random.truncated_normal(noise_key, -3.0, 3.0, (TOKENS, H * P_SIZE), jnp.float32)
    row_scale = jnp.exp(jax.random.uniform(row_key, (TOKENS, 1), jnp.float32, math.log(0.5), math.log(5.0)))
    column_scale = jnp.exp(jax.random.uniform(column_key, (1, H * P_SIZE), jnp.float32, math.log(0.5), math.log(5.0)))
    return (noise_draw * row_scale * column_scale).astype(jnp.bfloat16)


def draw_turn_first_token(key, part):
    per_block = TOK_DEV // UNIT
    block_count = TOKENS // TOK_DEV
    first_start = jax.random.randint(jax.random.fold_in(key, 201), (block_count,), 1, per_block - 1)
    first_start = jnp.where(jnp.arange(block_count) == 0, 0, first_start)
    room_left = per_block - 1 - first_start
    extra = jax.random.randint(jax.random.fold_in(key, 202), (block_count,), 0, 1 << 20) % room_left
    second_start = first_start + 1 + extra
    second_start = jnp.where(jnp.arange(block_count) == block_count - 1, per_block - 1, second_start)
    block_base = jnp.arange(block_count) * per_block
    joined = jnp.stack([block_base + first_start, block_base + second_start], axis=1)
    return (UNIT * joined).reshape(-1).astype(jnp.int32)


def set_ends(entries, own_key, least, high):
    place = [jax.random.randint(jax.random.fold_in(own_key, axis), (), 0, length) for axis, length in enumerate(entries.shape)]
    main_axis = entries.shape.index(max(entries.shape))
    neighbour = place[:main_axis] + [(place[main_axis] + 1) % entries.shape[main_axis]] + place[main_axis + 1:]
    return entries.at[tuple(place)].set(least).at[tuple(neighbour)].set(high)


def steps_of(rng, shape, shards, low, high):
    gain = 1.0
    for position, shards_of in shards:
        heights = jax.random.uniform(jax.random.fold_in(jax.random.fold_in(rng, 6), position), (shards_of,), jnp.float32, low / len(shards), high / len(shards))
        gain = gain * jnp.repeat(jnp.exp(heights), shape[position] // shards_of).reshape((-1,) + (1,) * (len(shape) - 1 - position))
    return gain


def rank_bounds(amount, slope):
    loads = [(1 << 20) // math.isqrt(grade ** slope) + 1 for grade in range(1, amount + 1)]
    deviation = 1 + sum(loads) // (1 << 30)
    return np.cumsum(np.array([max(1, weight // deviation) for weight in loads]))


def skewed_ids(stream_key, extent, count, slope):
    table = rank_bounds(count, slope)
    pick = jax.random.randint(jax.random.fold_in(stream_key, 1), extent, 0, int(table[count - 1]))
    grade = jnp.searchsorted(jnp.asarray(table, jnp.int32), pick, side="right")
    return jax.random.permutation(jax.random.fold_in(stream_key, 2), count)[grade].astype(jnp.int32)


def centred(rng, extent, deviation, most, cuts=(), held_as=jnp.bfloat16):
    gain = steps_of(rng, extent, cuts, -0.22, 0.18) if cuts else 1.0
    array = jax.random.normal(rng, extent, jnp.float32) * deviation * gain
    return jnp.minimum(jnp.maximum(array, -most), most).astype(held_as)


def setup_inputs(seed: int = 0) -> dict:
    keys = jax.random.split(jax.random.key(seed), 18)
    return {
        "input_x_channels": draw_input_x_channels(jax.random.fold_in(keys[17], 71), 0),
        "input_b_channels": centred(keys[1], (TOKENS, GN), 0.5, 3.0, ((0, 16), (1, 8))),
        "input_c_channels": centred(keys[2], (TOKENS, GN), 0.5, 3.0, ((0, 16), (1, 8))),
        "input_gate_channels": draw_input_gate_channels(jax.random.fold_in(keys[17], 71), 0),
        "raw_step_sizes": draw_raw_step_sizes(jax.random.fold_in(keys[17], 71), 0),
        "log_decay_rate": draw_log_decay_rate(jax.random.fold_in(keys[17], 71), 0),
        "head_skip_coeff": jnp.clip(0.5 + 1.5 * jax.random.uniform(keys[6], (H,), jnp.float32) ** steps_of(keys[6], (H,), ((0, 8),), -0.2, 0.2), 0.5, 2.0),
        "x_conv_taps": centred(keys[7], (K, INNER_CHANNELS), K ** -0.5, 3.0, ((1, 8),)),
        "b_conv_taps": centred(keys[8], (K, GN), K ** -0.5, 3.0, ((1, 8),)),
        "c_conv_taps": centred(keys[9], (K, GN), K ** -0.5, 3.0, ((1, 8),)),
        "gated_norm_gain": jnp.clip(1.0 + 0.18 * jax.random.normal(keys[10], (INNER_CHANNELS,), jnp.float32), 0.099609375, 1.8984375).astype(jnp.bfloat16),
        "output_weight": centred(keys[11], (INNER_CHANNELS, MODEL_WIDTH), INNER_CHANNELS ** -0.5, 0.0625, ((0, 8),)),
        "adapter_down_panels": centred(keys[12], (TENANT_COUNT, INNER_CHANNELS, ADAPTER_RANK), INNER_CHANNELS ** -0.5, 0.0625, ((0, 16), (1, 8))),
        "adapter_up_panels": centred(keys[13], (TENANT_COUNT, ADAPTER_RANK, MODEL_WIDTH), ADAPTER_RANK ** -0.5, 0.75, ((0, 16), (2, 8))),
        "turn_first_token": draw_turn_first_token(jax.random.fold_in(keys[17], 71), 0),
        "tenant_of_turn": set_ends(skewed_ids(keys[15], (TURNS,), TENANT_COUNT, 2), jax.random.fold_in(keys[15], 3), 0, TENANT_COUNT - 1).astype(jnp.int32),
        "tenant_panel_index": jax.random.permutation(keys[16], TENANT_COUNT).astype(jnp.int32),
    }


highest = lax.Precision.HIGHEST
epsilon = 1e-05

def conv_silu(sequence, weight):
    token_rows = sequence.shape[0]
    conv_edge = weight.shape[0] - 1
    joined = jnp.concatenate([jnp.zeros((conv_edge, sequence.shape[1]), jnp.float32), sequence.astype(jnp.float32)], axis=0)
    total = jnp.zeros((token_rows, sequence.shape[1]), jnp.float32)
    for tap in range(weight.shape[0]):
        total = total + weight[tap].astype(jnp.float32) * joined[tap:tap + token_rows]
    return jax.nn.silu(total).astype(jnp.bfloat16)

def group_layer(inputs):
    x_group, b_group, c_group, z_group, step_group, rate_group, skip_group, gain_group = inputs
    per_group = step_group.shape[0]
    token_rows = x_group.shape[0]
    block_count = token_rows // Q
    x_float = x_group.astype(jnp.float32).reshape(token_rows, per_group, P_SIZE)
    x_blocks = x_float.reshape(block_count, Q, per_group, P_SIZE)
    b_blocks = b_group.astype(jnp.float32).reshape(block_count, Q, N)
    c_blocks = c_group.astype(jnp.float32).reshape(block_count, Q, N)
    step_blocks = step_group.reshape(per_group, block_count, Q).transpose(1, 0, 2)
    running = jnp.cumsum(-step_blocks * rate_group[None, :, None], axis=2)
    causal = jnp.arange(Q)[:, None] >= jnp.arange(Q)[None, :]

    def advance(carried, block_span):
        x_part, b_part, c_part, step_part, run_part = block_span
        scores = jnp.dot(c_part, b_part.T, precision=highest)
        log_gap = run_part[:, :, None] - run_part[:, None, :]
        decay_mat = jnp.where(causal, jnp.exp(jnp.where(causal, log_gap, 0.0)), 0.0)
        mixing = scores[None] * decay_mat * step_part[:, None, :]
        output = jnp.einsum('hqk,khp->qhp', mixing, x_part, precision=highest)
        output = output + jnp.exp(run_part).T[:, :, None] * jnp.einsum('qn,hpn->qhp', c_part, carried, precision=highest)
        tail_weight = jnp.exp(run_part[:, -1:] - run_part) * step_part
        fresh = jnp.einsum('hk,khp,kn->hpn', tail_weight, x_part, b_part, precision=highest)
        return (jnp.exp(run_part[:, -1])[:, None, None] * carried + fresh, output)
    start = jnp.zeros((per_group, P_SIZE, N), jnp.float32)
    _, outputs = lax.scan(advance, start, (x_blocks, b_blocks, c_blocks, step_blocks, running))
    y_value = outputs.reshape(token_rows, per_group, P_SIZE) + skip_group[None, :, None] * x_float
    gated = y_value.reshape(token_rows, per_group * P_SIZE) * jax.nn.silu(z_group.astype(jnp.float32))
    norm_scale = lax.rsqrt(lax.optimization_barrier(jnp.mean(gated * gated, axis=1, keepdims=True)) + epsilon)
    return (gated * norm_scale * gain_group.astype(jnp.float32)).astype(jnp.bfloat16)

def reference(input_x_channels, input_b_channels, input_c_channels, input_gate_channels, raw_step_sizes, log_decay_rate, head_skip_coeff, x_conv_taps, b_conv_taps, c_conv_taps, gated_norm_gain, output_weight, adapter_down_panels, adapter_up_panels, turn_first_token, tenant_of_turn, tenant_panel_index):
    per_group = H // G
    group_width = per_group * P_SIZE
    x_conv = conv_silu(input_x_channels, x_conv_taps)
    b_conv = conv_silu(input_b_channels, b_conv_taps)
    c_conv = conv_silu(input_c_channels, c_conv_taps)
    step_sizes = jax.nn.softplus(raw_step_sizes)
    decay_rate = jnp.exp(log_decay_rate)
    grouped = (x_conv.reshape(TOKENS, G, group_width).transpose(1, 0, 2), b_conv.reshape(TOKENS, G, N).transpose(1, 0, 2), c_conv.reshape(TOKENS, G, N).transpose(1, 0, 2), input_gate_channels.reshape(TOKENS, G, group_width).transpose(1, 0, 2), step_sizes.reshape(G, per_group, TOKENS), decay_rate.reshape(G, per_group), head_skip_coeff.reshape(G, per_group), gated_norm_gain.reshape(G, group_width))
    normed = lax.map(group_layer, grouped)
    y_normed = normed.transpose(1, 0, 2).reshape(TOKENS, H * P_SIZE)
    base_out = jnp.dot(y_normed, output_weight, preferred_element_type=jnp.float32)

    def adapt(unit_index):
        first_token = unit_index * UNIT
        block_span = lax.dynamic_slice_in_dim(y_normed, first_token, UNIT, 0)
        turn_index = jnp.sum((turn_first_token <= first_token).astype(jnp.int32)) - 1
        panel_home_index = tenant_panel_index[tenant_of_turn[turn_index]]
        rank_reduced = jnp.dot(block_span, adapter_down_panels[panel_home_index], preferred_element_type=jnp.float32).astype(jnp.bfloat16)
        return jnp.dot(rank_reduced, adapter_up_panels[panel_home_index], preferred_element_type=jnp.float32)
    adapter_out = lax.map(adapt, jnp.arange(TOKENS // UNIT, dtype=jnp.int32)).reshape(TOKENS, MODEL_WIDTH)
    return (base_out + adapter_out).astype(jnp.bfloat16)
```

```python
import functools

import jax
import jax.numpy as jnp
from jax import lax
from jax.experimental import pallas as pl
from jax.experimental.pallas import tpu as pltpu
from jax.sharding import PartitionSpec as P

P_SIZE = 64
N = 128
Q = 128
TURN_DEV = 2
LOG2E = 1.4426950408889634
EPSILON = 1e-05
VMEM_LIMIT = 60 * 1024 * 1024
MESH = pl.DeviceIdType.MESH
F32 = jnp.float32
BF16 = jnp.bfloat16


def silu(v):
    half = 0.5 * v
    return half + half * jnp.tanh(half)


def dot(a, b):
    return jnp.dot(a, b, preferred_element_type=F32)


def dot_dims(a, b, ca, cb):
    return lax.dot_general(a, b, (((ca,), (cb,)), ((), ())), preferred_element_type=F32)


def scan_kernel(
    rate_ref, skip_ref, x_ref, b_ref, c_ref, z_ref, raw_ref, halo_ref, xt_ref, bt_ref, ct_ref,
    ylg_ref, eg_ref, cc_ref, s_ref, d_ref,
    xp, bp, cp, start, skl,
):
    step = pl.program_id(0)
    heads = raw_ref.shape[0]
    width = x_ref.shape[1]
    lane = lax.broadcasted_iota(jnp.int32, (8, 128), 1)

    @pl.when(step == 0)
    def _():
        xp[0:8, :] = halo_ref[:, 0:width].astype(F32)
        bp[0:8, :] = halo_ref[:, width : width + N].astype(F32)
        cp[0:8, :] = halo_ref[:, width + N : width + 2 * N].astype(F32)
        start[...] = jnp.zeros_like(start)
        s_ref[...] = jnp.zeros_like(s_ref)
        for pair in range(heads // 2):
            skl[:, pair * 128 : pair * 128 + 128] = jnp.where(
                lane < P_SIZE, skip_ref[2 * pair], skip_ref[2 * pair + 1]
            )

    @pl.when(step > 0)
    def _():
        xp[0:8, :] = xp[Q : Q + 8, :]
        bp[0:8, :] = bp[Q : Q + 8, :]
        cp[0:8, :] = cp[Q : Q + 8, :]

    xp[8 : 8 + Q, :] = x_ref[...].astype(F32)
    bp[8 : 8 + Q, :] = b_ref[...].astype(F32)
    cp[8 : 8 + Q, :] = c_ref[...].astype(F32)

    def conv(padded, taps, sl):
        total = taps[0:1, sl].astype(F32) * padded[5 : 5 + Q, sl]
        for k in range(1, 4):
            total = total + taps[k : k + 1, sl].astype(F32) * padded[5 + k : 5 + k + Q, sl]
        return silu(total).astype(BF16)

    every = slice(0, N)
    bc = conv(bp, bt_ref, every)
    cc = conv(cp, ct_ref, every)
    cc_ref[...] = cc
    bt = bc.astype(F32).T.astype(BF16)
    row = lax.broadcasted_iota(jnp.int32, (Q, Q), 0)
    col = lax.broadcasted_iota(jnp.int32, (Q, Q), 1)
    scores = jnp.where(row >= col, dot(cc, bt), 0.0)

    raw = raw_ref[...]
    dt = jnp.maximum(raw, 0.0) + jnp.log1p(jnp.exp(-jnp.abs(raw)))
    hrow = lax.broadcasted_iota(jnp.int32, (heads, Q), 0)
    lrow = lax.broadcasted_iota(jnp.int32, (heads, Q), 1)
    rate = jnp.zeros((heads, Q), F32)
    for h in range(heads):
        rate = jnp.where(hrow == h, rate_ref[h], rate)
    run = -dt * jnp.exp(rate)
    shift = 1
    while shift < Q:
        run = run + jnp.where(lrow >= shift, pltpu.roll(run, shift, 1), 0.0)
        shift *= 2
    run2 = run * LOG2E
    last2 = jnp.broadcast_to(run2[:, Q - 1 : Q], (heads, Q))
    stacked = jnp.concatenate(
        [dt, run2] + [jnp.zeros((heads, Q), F32)] * ((Q - 2 * heads) // heads), axis=0
    )
    tr = stacked.T
    before2 = start[...]
    start[...] = before2 + last2
    half_lane = lax.broadcasted_iota(jnp.int32, (Q, 128), 1) < P_SIZE
    half_row = lax.broadcasted_iota(jnp.int32, (1, 128), 1) < P_SIZE

    for pair in range(heads // 2):
        h0, h1 = 2 * pair, 2 * pair + 1
        sl = slice(pair * 128, pair * 128 + 128)
        xc = conv(xp, xt_ref, sl).astype(F32)
        dt_e = jnp.where(half_lane, tr[:, h0 : h0 + 1], tr[:, h1 : h1 + 1])
        c0 = jnp.broadcast_to(tr[:, heads + h0 : heads + h0 + 1], (Q, Q))
        c1 = jnp.broadcast_to(tr[:, heads + h1 : heads + h1 + 1], (Q, Q))
        run_e = jnp.where(half_lane, c0, c1)
        last_e = jnp.where(half_row, last2[h0 : h0 + 1, :], last2[h1 : h1 + 1, :])
        start_e = jnp.where(half_row, before2[h0 : h0 + 1, :], before2[h1 : h1 + 1, :])
        xdt = xc * dt_e
        m0 = (scores * jnp.exp2(jnp.minimum(c0 - run2[h0 : h0 + 1, :], 0.0))).astype(BF16)
        m1 = (scores * jnp.exp2(jnp.minimum(c1 - run2[h1 : h1 + 1, :], 0.0))).astype(BF16)
        mixing = jnp.concatenate([m0, m1], axis=1)
        xdt_pair = jnp.concatenate(
            [jnp.where(half_lane, xdt, 0.0), jnp.where(half_lane, 0.0, xdt)], axis=0
        ).astype(BF16)
        grow = jnp.exp2(run_e)
        carried = s_ref[:, sl]
        y = dot(mixing, xdt_pair) + grow * dot(cc, carried.astype(BF16)) + skl[0:1, sl] * xc
        gate = silu(z_ref[:, sl].astype(F32))
        ylg_ref[:, sl] = (y * gate).astype(BF16)
        eg_ref[:, sl] = (grow * jnp.exp2(start_e) * gate).astype(BF16)
        weighted = (xdt * jnp.exp2(last_e - run_e)).astype(BF16)
        s_ref[:, sl] = jnp.exp2(last_e) * carried + dot(bt, weighted)
        d_ref[:, sl] = jnp.broadcast_to(jnp.exp2(start_e + last_e), (8, 128))


def local_scan(x, b, c, z, raw, rate, skip, halo, xt, bt, ct):
    tokens, width = x.shape
    heads = raw.shape[0]
    smem = pl.BlockSpec(memory_space=pltpu.SMEM)
    whole = lambda a: pl.BlockSpec(a.shape, lambda i: (0,) * a.ndim)
    rows = lambda w: pl.BlockSpec((Q, w), lambda i: (i, 0))
    return pl.pallas_call(
        scan_kernel,
        grid=(tokens // Q,),
        in_specs=[
            smem, smem, rows(width), rows(N), rows(N), rows(width),
            pl.BlockSpec((heads, Q), lambda i: (0, i)),
            whole(halo), whole(xt), whole(bt), whole(ct),
        ],
        out_specs=[
            rows(width), rows(width), rows(N),
            pl.BlockSpec((N, width), lambda i: (0, 0)),
            pl.BlockSpec((8, width), lambda i: (0, 0)),
        ],
        out_shape=[
            jax.ShapeDtypeStruct((tokens, width), BF16),
            jax.ShapeDtypeStruct((tokens, width), BF16),
            jax.ShapeDtypeStruct((tokens, N), BF16),
            jax.ShapeDtypeStruct((N, width), F32),
            jax.ShapeDtypeStruct((8, width), F32),
        ],
        scratch_shapes=[
            pltpu.VMEM((Q + 8, width), F32),
            pltpu.VMEM((Q + 8, N), F32),
            pltpu.VMEM((Q + 8, N), F32),
            pltpu.VMEM((heads, Q), F32),
            pltpu.VMEM((8, width), F32),
        ],
        compiler_params=pltpu.CompilerParams(
            dimension_semantics=("arbitrary",), vmem_limit_bytes=VMEM_LIMIT
        ),
        name="local_scan",
    )(rate, skip, x, b, c, z, raw, halo, xt, bt, ct)


def partners():
    me = lax.axis_index("ctx")
    x, z = me // 4, me % 4
    return [
        (x * 4 + (z + 1 - 2 * (z % 2)), z % 2),
        (x * 4 + (3 - z), z // 2),
        ((x + 1 - 2 * (x % 2)) * 4 + z, x % 2),
        ((3 - x) * 4 + z, x // 2),
    ]


def exchange_kernel(
    s_ref, d_ref, inc_ref, total, prefix, decay, dsend, drecv, ssend, srecv,
    sem_ds, sem_dr, sem_ss, sem_sr, *, chunks,
):
    steps = partners()
    barrier = pltpu.get_barrier_semaphore()
    for other, _ in steps:
        pl.semaphore_signal(barrier, inc=1, device_id={"ctx": other}, device_id_type=MESH)
    width = s_ref.shape[1]
    cw = width // chunks

    def state_copy(c, s):
        return pltpu.make_async_remote_copy(
            src_ref=ssend.at[s, c], dst_ref=srecv.at[s, c],
            send_sem=sem_ss.at[s, c], recv_sem=sem_sr.at[s, c],
            device_id={"ctx": steps[s][0]}, device_id_type=MESH,
        )

    def decay_copy(s):
        return pltpu.make_async_remote_copy(
            src_ref=dsend.at[s], dst_ref=drecv.at[s],
            send_sem=sem_ds.at[s], recv_sem=sem_dr.at[s],
            device_id={"ctx": steps[s][0]}, device_id_type=MESH,
        )

    for c in range(chunks):
        ssend[0, c] = s_ref[:, c * cw : c * cw + cw].astype(BF16)
    dsend[0] = d_ref[...]
    total[...] = s_ref[...]
    prefix[...] = jnp.zeros_like(prefix)
    pl.semaphore_wait(barrier, len(steps))
    decay_copy(0).start()
    for c in range(chunks):
        state_copy(c, 0).start()
    decay[0] = d_ref[...]
    decay[1] = jnp.ones_like(d_ref)
    for wave in range(chunks + 3):
        for s in range(4):
            c = wave - s
            if c < 0 or c >= chunks:
                continue
            sl = slice(c * cw, c * cw + cw)
            upper = steps[s][1] == 1
            if c == 0:
                decay_copy(s).wait_recv()
                theirs = drecv[s]
                decay[2 * s + 2] = decay[2 * s] * theirs
                decay[2 * s + 3] = decay[2 * s + 1] * jnp.where(upper, theirs, 1.0)
                if s < 3:
                    dsend[s + 1] = decay[2 * s + 2]
                    decay_copy(s + 1).start()
            state_copy(c, s).wait_recv()
            incoming = srecv[s, c].astype(F32)
            mine = decay[2 * s, 0:1, sl]
            ahead = decay[2 * s + 1, 0:1, sl]
            theirs = drecv[s, 0:1, sl]
            prefix[:, sl] = prefix[:, sl] + jnp.where(upper, ahead, 0.0) * incoming
            if s < 3:
                new = (
                    jnp.where(upper, mine, 1.0) * incoming
                    + jnp.where(upper, 1.0, theirs) * total[:, sl]
                )
                total[:, sl] = new
                ssend[s + 1, c] = new.astype(BF16)
                state_copy(c, s + 1).start()
    inc_ref[...] = prefix[...].astype(BF16)
    for s in range(4):
        decay_copy(s).wait_send()
        for c in range(chunks):
            state_copy(c, s).wait_send()


def exchange(state, decay, chunks=8):
    width = state.shape[1]
    cw = width // chunks
    vmem = pl.BlockSpec(memory_space=pltpu.VMEM)
    return pl.pallas_call(
        functools.partial(exchange_kernel, chunks=chunks),
        in_specs=[vmem, vmem],
        out_specs=vmem,
        out_shape=jax.ShapeDtypeStruct((N, width), BF16),
        scratch_shapes=[
            pltpu.VMEM((N, width), F32),
            pltpu.VMEM((N, width), F32),
            pltpu.VMEM((10, 8, width), F32),
            pltpu.VMEM((4, 8, width), F32),
            pltpu.VMEM((4, 8, width), F32),
            pltpu.VMEM((4, chunks, N, cw), BF16),
            pltpu.VMEM((4, chunks, N, cw), BF16),
            pltpu.SemaphoreType.DMA((4,)),
            pltpu.SemaphoreType.DMA((4,)),
            pltpu.SemaphoreType.DMA((4, chunks)),
            pltpu.SemaphoreType.DMA((4, chunks)),
        ],
        compiler_params=pltpu.CompilerParams(
            collective_id=1, has_side_effects=True, vmem_limit_bytes=VMEM_LIMIT
        ),
        name="state_exchange",
    )(state, decay)


LAG = (1, 2, 3, 4)


def project_kernel(
    slot_ref, ylg_ref, eg_ref, cc_ref, inc_ref, gain_ref, down_ref, w_ref,
    base_ref, low_ref,
    wv, own, psend, precv, rsend, rrecv, lsend, lrecv, lout,
    sem_w, sem_ps, sem_pr, sem_rs, sem_rr, sem_ls, sem_lr, sem_as, sem_ar,
):
    head = lax.axis_index("head")
    y, core = head // 2, head % 2
    blocks = ylg_ref.shape[0] // Q
    feat = base_ref.shape[1]
    half = Q // 2
    barrier = pltpu.get_barrier_semaphore()
    for k in range(1, 8):
        pl.semaphore_signal(
            barrier, inc=1, device_id={"head": (head + k) % 8}, device_id_type=MESH
        )

    dests = [(y + 3) % 4, (y + 1) % 4, (y + 2) % 4, y]

    def w_copy(d, side):
        index = d * 2 + side
        at = pl.multiple_of(index * feat, feat)
        return pltpu.make_async_copy(w_ref.at[:, pl.ds(at, feat)], wv.at[index], sem_w.at[index])

    for d in dests:
        for side in (1 - core, core):
            w_copy(d, side).start()

    def pair_copy(b, d):
        return pltpu.make_async_remote_copy(
            src_ref=psend.at[b, d], dst_ref=precv.at[b, d],
            send_sem=sem_ps.at[b, d], recv_sem=sem_pr.at[b, d],
            device_id={"head": y * 2 + 1 - core}, device_id_type=MESH,
        )

    def ring_copy(b, j, way):
        to = (y + 1 + 2 * way) % 4
        return pltpu.make_async_remote_copy(
            src_ref=rsend.at[b, j, way], dst_ref=rrecv.at[b, j, way],
            send_sem=sem_rs.at[b, j, way], recv_sem=sem_rr.at[b, j, way],
            device_id={"head": to * 2 + core}, device_id_type=MESH,
        )

    def low_copy(b):
        return pltpu.make_async_remote_copy(
            src_ref=lsend.at[b], dst_ref=lrecv.at[head],
            send_sem=sem_ls.at[b], recv_sem=sem_lr.at[head],
            device_id={"head": b}, device_id_type=MESH,
        )

    def low_arrival(k):
        return pltpu.make_async_remote_copy(
            src_ref=lsend.at[k], dst_ref=lrecv.at[k],
            send_sem=sem_ls.at[k], recv_sem=sem_lr.at[k],
            device_id={"head": k}, device_id_type=MESH,
        )

    def sum_copy(k):
        return pltpu.make_async_remote_copy(
            src_ref=lout.at[head], dst_ref=lout.at[head],
            send_sem=sem_as.at[k], recv_sem=sem_ar.at[head],
            device_id={"head": k}, device_id_type=MESH,
        )

    def sum_arrival(k):
        return pltpu.make_async_remote_copy(
            src_ref=lout.at[k], dst_ref=lout.at[k],
            send_sem=sem_as.at[k], recv_sem=sem_ar.at[k],
            device_id={"head": k}, device_id_type=MESH,
        )

    pl.semaphore_wait(barrier, 7)

    def compute(b):
        rows = pl.ds(pl.multiple_of(b * Q, Q), Q)
        got = dot(cc_ref[rows, :], inc_ref[...])
        gated = ylg_ref[rows, :].astype(F32) + eg_ref[rows, :].astype(F32) * got
        scale = lax.rsqrt(jnp.mean(gated * gated, axis=1, keepdims=True) + EPSILON)
        normed = (gated * scale * gain_ref[...].astype(F32)).astype(BF16)
        for d in dests:
            @pl.when(b == 0)
            def _():
                w_copy(d, 1 - core).wait()
            psend[b, d] = dot(normed, wv[d * 2 + 1 - core]).astype(BF16)
            pair_copy(b, d).start()

            @pl.when(b == 0)
            def _():
                w_copy(d, core).wait()
            own[b, d] = dot(normed, wv[d * 2 + core])
        low = dot_dims(down_ref[slot_ref[b]], normed, 1, 1).astype(BF16)
        lsend[b] = low

        @pl.when(b == head)
        def _():
            lrecv[b] = low

        @pl.when(b != head)
        def _():
            low_copy(b).start()

    def ring(b, j):
        if j == 0:
            pair_copy(b, dests[0]).wait_recv()
            pair_copy(b, dests[1]).wait_recv()
        elif j == 1:
            pair_copy(b, dests[2]).wait_recv()
        elif j == 3:
            pair_copy(b, dests[3]).wait_recv()
        for way in range(2):
            d = (y + (j + 1) * (3 - 2 * way)) % 4
            part = slice(way * half, way * half + half)
            value = own[b, d, part, :] + precv[b, d, part, :].astype(F32)
            if j > 0:
                ring_copy(b, j - 1, way).wait_recv()
                value = value + rrecv[b, j - 1, way].astype(F32)
            if j < 3:
                rsend[b, j, way] = value.astype(BF16)
                ring_copy(b, j, way).start()
            else:
                at = pl.multiple_of(b * Q + way * half, half)
                base_ref[pl.ds(at, half), :] = value

    def sum_low():
        for k in range(8):
            @pl.when(k != head)
            def _():
                low_arrival(k).wait_recv()
        total = lrecv[0].astype(F32)
        for k in range(1, 8):
            total = total + lrecv[k].astype(F32)
        lout[head] = total.astype(BF16)
        for k in range(8):
            @pl.when(k != head)
            def _():
                sum_copy(k).start()

    def tick(t, carry):
        @pl.when(t < blocks)
        def _():
            compute(t)

        for j in range(4):
            b = t - LAG[j]

            @pl.when(jnp.logical_and(b >= 0, b < blocks))
            def _():
                ring(b, j)

        @pl.when(t == blocks + 1)
        def _():
            sum_low()

        return carry

    lax.fori_loop(0, blocks + LAG[3], tick, 0)

    for k in range(8):
        @pl.when(k != head)
        def _():
            sum_arrival(k).wait_recv()
            low_copy(k).wait_send()
            sum_copy(k).wait_send()
    low_ref[...] = lout[...]

    def drain(b, carry):
        for d in range(4):
            pair_copy(b, d).wait_send()
        for j in range(3):
            for way in range(2):
                ring_copy(b, j, way).wait_send()
        return carry

    lax.fori_loop(0, blocks, drain, 0)


def project(slots, ylg, eg, cc, inc, gain, down, weight):
    tokens, width = ylg.shape
    feat = weight.shape[1] // 8
    rank = down.shape[1]
    blocks = tokens // Q
    vmem = pl.BlockSpec(memory_space=pltpu.VMEM)
    dma = pltpu.SemaphoreType.DMA
    return pl.pallas_call(
        project_kernel,
        in_specs=[pl.BlockSpec(memory_space=pltpu.SMEM)] + [vmem] * 6 + [pl.BlockSpec(memory_space=pl.ANY)],
        out_specs=[vmem, vmem],
        out_shape=[
            jax.ShapeDtypeStruct((tokens, feat), F32),
            jax.ShapeDtypeStruct((blocks, rank, Q), BF16),
        ],
        scratch_shapes=[
            pltpu.VMEM((8, width, feat), BF16),
            pltpu.VMEM((blocks, 4, Q, feat), F32),
            pltpu.VMEM((blocks, 4, Q, feat), BF16),
            pltpu.VMEM((blocks, 4, Q, feat), BF16),
            pltpu.VMEM((blocks, 3, 2, Q // 2, feat), BF16),
            pltpu.VMEM((blocks, 3, 2, Q // 2, feat), BF16),
            pltpu.VMEM((8, rank, Q), BF16),
            pltpu.VMEM((8, rank, Q), BF16),
            pltpu.VMEM((8, rank, Q), BF16),
            dma((8,)), dma((blocks, 4)), dma((blocks, 4)), dma((blocks, 3, 2)), dma((blocks, 3, 2)),
            dma((8,)), dma((8,)), dma((8,)), dma((8,)),
        ],
        compiler_params=pltpu.CompilerParams(
            collective_id=2, has_side_effects=True, vmem_limit_bytes=VMEM_LIMIT
        ),
        name="project",
    )(slots, ylg, eg, cc, inc, gain, down, weight)


def adapt_kernel(slot_ref, base_ref, low_ref, up_ref, out_ref):
    out_ref[...] = (base_ref[...] + dot_dims(low_ref[0], up_ref[0], 0, 0)).astype(BF16)


def adapt(slots, base, low, up):
    tokens, feat = base.shape
    rank = low.shape[1]
    return pl.pallas_call(
        adapt_kernel,
        grid_spec=pltpu.PrefetchScalarGridSpec(
            num_scalar_prefetch=1,
            grid=(tokens // Q,),
            in_specs=[
                pl.BlockSpec((Q, feat), lambda i, s: (i, 0)),
                pl.BlockSpec((1, rank, Q), lambda i, s: (i, 0, 0)),
                pl.BlockSpec((1, rank, feat), lambda i, s: (s[i], 0, 0)),
            ],
            out_specs=pl.BlockSpec((Q, feat), lambda i, s: (i, 0)),
        ),
        out_shape=jax.ShapeDtypeStruct((tokens, feat), BF16),
        compiler_params=pltpu.CompilerParams(vmem_limit_bytes=16 * 1024 * 1024),
        name="adapt",
    )(slots, base, low, up)


def local(
    input_x_channels,
    input_b_channels,
    input_c_channels,
    input_gate_channels,
    raw_step_sizes,
    log_decay_rate,
    head_skip_coeff,
    x_conv_taps,
    b_conv_taps,
    c_conv_taps,
    gated_norm_gain,
    output_weight,
    adapter_down_panels,
    adapter_up_panels,
    turn_first_token,
    tenant_of_turn,
    tenant_panel_index,
):
    tokens = input_x_channels.shape[0]
    own = lax.axis_index("ctx")
    slot_turns = jnp.maximum(TURN_DEV * own - 1 + jnp.arange(TURN_DEV + 1), 0)
    homes = jnp.take(tenant_panel_index, jnp.take(tenant_of_turn, slot_turns))
    starts = lax.dynamic_slice_in_dim(turn_first_token, TURN_DEV * own, TURN_DEV, 0)
    places = own * tokens + Q * jnp.arange(tokens // Q)
    slots = jnp.sum((places[:, None] >= starts[None, :]).astype(jnp.int32), axis=1)

    all_down = lax.all_gather(adapter_down_panels.transpose(0, 2, 1), "ctx", axis=0, tiled=True)
    all_up = lax.all_gather(adapter_up_panels, "ctx", axis=0, tiled=True)
    down = jnp.take(all_down, homes, axis=0)
    up = jnp.take(all_up, homes, axis=0)

    tails = jnp.concatenate(
        [input_x_channels[tokens - 8 :], input_b_channels[tokens - 8 :], input_c_channels[tokens - 8 :]],
        axis=1,
    )
    count = lax.axis_size("ctx")
    halo = lax.ppermute(tails, "ctx", [(i, i + 1) for i in range(count - 1)])
    ylg, eg, cc, state, decay = local_scan(
        input_x_channels, input_b_channels, input_c_channels, input_gate_channels, raw_step_sizes,
        log_decay_rate, head_skip_coeff, halo, x_conv_taps, b_conv_taps, c_conv_taps,
    )
    inc = exchange(state, decay)
    base, low = project(slots, ylg, eg, cc, inc, gated_norm_gain.reshape(1, -1), down, output_weight)
    return adapt(slots, base, low, up)


def solution(mesh):
    in_specs = (
        P("ctx", "head"),
        P("ctx", "head"),
        P("ctx", "head"),
        P("ctx", "head"),
        P("head", "ctx"),
        P("head"),
        P("head"),
        P(None, "head"),
        P(None, "head"),
        P(None, "head"),
        P("head"),
        P("head", None),
        P("ctx", "head", None),
        P("ctx", None, "head"),
        P(),
        P(),
        P(),
    )
    out_specs = P("ctx", "head")
    return jax.shard_map(local, mesh=mesh, in_specs=in_specs, out_specs=out_specs, check_vma=False)
```

```python
import functools

import jax
import jax.numpy as jnp
from jax import lax
from jax.experimental import pallas as pl
from jax.experimental.pallas import tpu as pltpu
from jax.sharding import PartitionSpec as P

P_SIZE = 64
N = 128
Q = 128
TURN_DEV = 2
PANEL_DEV = 6
LOG2E = 1.4426950408889634
EPSILON = 1e-05
VMEM_LIMIT = 60 * 1024 * 1024
MESH = pl.DeviceIdType.MESH
F32 = jnp.float32
BF16 = jnp.bfloat16


def silu(v):
    half = 0.5 * v
    return half + half * jnp.tanh(half)


def dot(a, b):
    return jnp.dot(a, b, preferred_element_type=F32)


def dot_dims(a, b, ca, cb):
    return lax.dot_general(a, b, (((ca,), (cb,)), ((), ())), preferred_element_type=F32)


def scan_kernel(
    rate_ref, skip_ref, x_ref, b_ref, c_ref, z_ref, raw_ref, halo_ref, xt_ref, bt_ref, ct_ref,
    ylg_ref, eg_ref, cc_ref, s_ref, d_ref,
    xp, bp, cp, start, skl,
):
    step = pl.program_id(0)
    heads = raw_ref.shape[0]
    width = x_ref.shape[1]
    lane = lax.broadcasted_iota(jnp.int32, (8, 128), 1)

    @pl.when(step == 0)
    def _():
        xp[0:8, :] = halo_ref[:, 0:width].astype(F32)
        bp[0:8, :] = halo_ref[:, width : width + N].astype(F32)
        cp[0:8, :] = halo_ref[:, width + N : width + 2 * N].astype(F32)
        start[...] = jnp.zeros_like(start)
        s_ref[...] = jnp.zeros_like(s_ref)
        for pair in range(heads // 2):
            skl[:, pair * 128 : pair * 128 + 128] = jnp.where(
                lane < P_SIZE, skip_ref[2 * pair], skip_ref[2 * pair + 1]
            )

    @pl.when(step > 0)
    def _():
        xp[0:8, :] = xp[Q : Q + 8, :]
        bp[0:8, :] = bp[Q : Q + 8, :]
        cp[0:8, :] = cp[Q : Q + 8, :]

    xp[8 : 8 + Q, :] = x_ref[...].astype(F32)
    bp[8 : 8 + Q, :] = b_ref[...].astype(F32)
    cp[8 : 8 + Q, :] = c_ref[...].astype(F32)

    def conv(padded, taps, sl):
        total = taps[0:1, sl].astype(F32) * padded[5 : 5 + Q, sl]
        for k in range(1, 4):
            total = total + taps[k : k + 1, sl].astype(F32) * padded[5 + k : 5 + k + Q, sl]
        return silu(total).astype(BF16)

    every = slice(0, N)
    bc = conv(bp, bt_ref, every)
    cc = conv(cp, ct_ref, every)
    cc_ref[...] = cc
    bt = bc.astype(F32).T.astype(BF16)
    row = lax.broadcasted_iota(jnp.int32, (Q, Q), 0)
    col = lax.broadcasted_iota(jnp.int32, (Q, Q), 1)
    scores = jnp.where(row >= col, dot(cc, bt), 0.0)

    raw = raw_ref[...]
    dt = jnp.maximum(raw, 0.0) + jnp.log1p(jnp.exp(-jnp.abs(raw)))
    hrow = lax.broadcasted_iota(jnp.int32, (heads, Q), 0)
    lrow = lax.broadcasted_iota(jnp.int32, (heads, Q), 1)
    rate = jnp.zeros((heads, Q), F32)
    for h in range(heads):
        rate = jnp.where(hrow == h, rate_ref[h], rate)
    run = -dt * jnp.exp(rate)
    shift = 1
    while shift < Q:
        run = run + jnp.where(lrow >= shift, pltpu.roll(run, shift, 1), 0.0)
        shift *= 2
    run2 = run * LOG2E
    last2 = jnp.broadcast_to(run2[:, Q - 1 : Q], (heads, Q))
    stacked = jnp.concatenate(
        [dt, run2] + [jnp.zeros((heads, Q), F32)] * ((Q - 2 * heads) // heads), axis=0
    )
    tr = stacked.T
    before2 = start[...]
    start[...] = before2 + last2
    half_lane = lax.broadcasted_iota(jnp.int32, (Q, 128), 1) < P_SIZE
    half_row = lax.broadcasted_iota(jnp.int32, (1, 128), 1) < P_SIZE

    for pair in range(heads // 2):
        h0, h1 = 2 * pair, 2 * pair + 1
        sl = slice(pair * 128, pair * 128 + 128)
        xc = conv(xp, xt_ref, sl).astype(F32)
        dt_e = jnp.where(half_lane, tr[:, h0 : h0 + 1], tr[:, h1 : h1 + 1])
        c0 = jnp.broadcast_to(tr[:, heads + h0 : heads + h0 + 1], (Q, Q))
        c1 = jnp.broadcast_to(tr[:, heads + h1 : heads + h1 + 1], (Q, Q))
        run_e = jnp.where(half_lane, c0, c1)
        last_e = jnp.where(half_row, last2[h0 : h0 + 1, :], last2[h1 : h1 + 1, :])
        start_e = jnp.where(half_row, before2[h0 : h0 + 1, :], before2[h1 : h1 + 1, :])
        xdt = xc * dt_e
        m0 = (scores * jnp.exp2(jnp.minimum(c0 - run2[h0 : h0 + 1, :], 0.0))).astype(BF16)
        m1 = (scores * jnp.exp2(jnp.minimum(c1 - run2[h1 : h1 + 1, :], 0.0))).astype(BF16)
        mixing = jnp.concatenate([m0, m1], axis=1)
        xdt_pair = jnp.concatenate(
            [jnp.where(half_lane, xdt, 0.0), jnp.where(half_lane, 0.0, xdt)], axis=0
        ).astype(BF16)
        grow = jnp.exp2(run_e)
        carried = s_ref[:, sl]
        y = dot(mixing, xdt_pair) + grow * dot(cc, carried.astype(BF16)) + skl[0:1, sl] * xc
        gate = silu(z_ref[:, sl].astype(F32))
        ylg_ref[:, sl] = (y * gate).astype(BF16)
        eg_ref[:, sl] = (grow * jnp.exp2(start_e) * gate).astype(BF16)
        weighted = (xdt * jnp.exp2(last_e - run_e)).astype(BF16)
        s_ref[:, sl] = jnp.exp2(last_e) * carried + dot(bt, weighted)
        d_ref[:, sl] = jnp.broadcast_to(jnp.exp2(start_e + last_e), (8, 128))


def local_scan(x, b, c, z, raw, rate, skip, halo, xt, bt, ct):
    tokens, width = x.shape
    heads = raw.shape[0]
    smem = pl.BlockSpec(memory_space=pltpu.SMEM)
    whole = lambda a: pl.BlockSpec(a.shape, lambda i: (0,) * a.ndim)
    rows = lambda w: pl.BlockSpec((Q, w), lambda i: (i, 0))
    return pl.pallas_call(
        scan_kernel,
        grid=(tokens // Q,),
        in_specs=[
            smem, smem, rows(width), rows(N), rows(N), rows(width),
            pl.BlockSpec((heads, Q), lambda i: (0, i)),
            whole(halo), whole(xt), whole(bt), whole(ct),
        ],
        out_specs=[
            rows(width), rows(width), rows(N),
            pl.BlockSpec((N, width), lambda i: (0, 0)),
            pl.BlockSpec((8, width), lambda i: (0, 0)),
        ],
        out_shape=[
            jax.ShapeDtypeStruct((tokens, width), BF16),
            jax.ShapeDtypeStruct((tokens, width), BF16),
            jax.ShapeDtypeStruct((tokens, N), BF16),
            jax.ShapeDtypeStruct((N, width), F32),
            jax.ShapeDtypeStruct((8, width), F32),
        ],
        scratch_shapes=[
            pltpu.VMEM((Q + 8, width), F32),
            pltpu.VMEM((Q + 8, N), F32),
            pltpu.VMEM((Q + 8, N), F32),
            pltpu.VMEM((heads, Q), F32),
            pltpu.VMEM((8, width), F32),
        ],
        compiler_params=pltpu.CompilerParams(
            dimension_semantics=("arbitrary",), vmem_limit_bytes=VMEM_LIMIT
        ),
        name="local_scan",
    )(rate, skip, x, b, c, z, raw, halo, xt, bt, ct)


def partners():
    me = lax.axis_index("ctx")
    x, z = me // 4, me % 4
    return [
        (x * 4 + (z + 1 - 2 * (z % 2)), z % 2),
        (x * 4 + (3 - z), z // 2),
        ((x + 1 - 2 * (x % 2)) * 4 + z, x % 2),
        ((3 - x) * 4 + z, x // 2),
    ]


def exchange_kernel(
    s_ref, d_ref, inc_ref, total, prefix, decay, dsend, drecv, ssend, srecv,
    sem_ds, sem_dr, sem_ss, sem_sr, *, chunks,
):
    steps = partners()
    barrier = pltpu.get_barrier_semaphore()
    for other, _ in steps:
        pl.semaphore_signal(barrier, inc=1, device_id={"ctx": other}, device_id_type=MESH)
    width = s_ref.shape[1]
    cw = width // chunks

    def state_copy(c, s):
        return pltpu.make_async_remote_copy(
            src_ref=ssend.at[s, c], dst_ref=srecv.at[s, c],
            send_sem=sem_ss.at[s, c], recv_sem=sem_sr.at[s, c],
            device_id={"ctx": steps[s][0]}, device_id_type=MESH,
        )

    def decay_copy(s):
        return pltpu.make_async_remote_copy(
            src_ref=dsend.at[s], dst_ref=drecv.at[s],
            send_sem=sem_ds.at[s], recv_sem=sem_dr.at[s],
            device_id={"ctx": steps[s][0]}, device_id_type=MESH,
        )

    for c in range(chunks):
        ssend[0, c] = s_ref[:, c * cw : c * cw + cw].astype(BF16)
    dsend[0] = d_ref[...]
    total[...] = s_ref[...]
    prefix[...] = jnp.zeros_like(prefix)
    pl.semaphore_wait(barrier, len(steps))
    decay_copy(0).start()
    for c in range(chunks):
        state_copy(c, 0).start()
    decay[0] = d_ref[...]
    decay[1] = jnp.ones_like(d_ref)
    for wave in range(chunks + 3):
        for s in range(4):
            c = wave - s
            if c < 0 or c >= chunks:
                continue
            sl = slice(c * cw, c * cw + cw)
            upper = steps[s][1] == 1
            if c == 0:
                decay_copy(s).wait_recv()
                theirs = drecv[s]
                decay[2 * s + 2] = decay[2 * s] * theirs
                decay[2 * s + 3] = decay[2 * s + 1] * jnp.where(upper, theirs, 1.0)
                if s < 3:
                    dsend[s + 1] = decay[2 * s + 2]
                    decay_copy(s + 1).start()
            state_copy(c, s).wait_recv()
            incoming = srecv[s, c].astype(F32)
            mine = decay[2 * s, 0:1, sl]
            ahead = decay[2 * s + 1, 0:1, sl]
            theirs = drecv[s, 0:1, sl]
            prefix[:, sl] = prefix[:, sl] + jnp.where(upper, ahead, 0.0) * incoming
            if s < 3:
                new = (
                    jnp.where(upper, mine, 1.0) * incoming
                    + jnp.where(upper, 1.0, theirs) * total[:, sl]
                )
                total[:, sl] = new
                ssend[s + 1, c] = new.astype(BF16)
                state_copy(c, s + 1).start()
    inc_ref[...] = prefix[...].astype(BF16)
    for s in range(4):
        decay_copy(s).wait_send()
        for c in range(chunks):
            state_copy(c, s).wait_send()


def exchange(state, decay, chunks=8):
    width = state.shape[1]
    cw = width // chunks
    vmem = pl.BlockSpec(memory_space=pltpu.VMEM)
    return pl.pallas_call(
        functools.partial(exchange_kernel, chunks=chunks),
        in_specs=[vmem, vmem],
        out_specs=vmem,
        out_shape=jax.ShapeDtypeStruct((N, width), BF16),
        scratch_shapes=[
            pltpu.VMEM((N, width), F32),
            pltpu.VMEM((N, width), F32),
            pltpu.VMEM((10, 8, width), F32),
            pltpu.VMEM((4, 8, width), F32),
            pltpu.VMEM((4, 8, width), F32),
            pltpu.VMEM((4, chunks, N, cw), BF16),
            pltpu.VMEM((4, chunks, N, cw), BF16),
            pltpu.SemaphoreType.DMA((4,)),
            pltpu.SemaphoreType.DMA((4,)),
            pltpu.SemaphoreType.DMA((4, chunks)),
            pltpu.SemaphoreType.DMA((4, chunks)),
        ],
        compiler_params=pltpu.CompilerParams(
            collective_id=1, has_side_effects=True, vmem_limit_bytes=VMEM_LIMIT
        ),
        name="state_exchange",
    )(state, decay)


LAG = (1, 2, 3, 4)


def project_kernel(
    slot_ref, ylg_ref, eg_ref, cc_ref, inc_ref, gain_ref, down_ref, w_ref,
    base_ref, low_ref,
    wv, own, psend, precv, rsend, rrecv, lsend, lrecv, lout,
    sem_w, sem_ps, sem_pr, sem_rs, sem_rr, sem_ls, sem_lr, sem_as, sem_ar,
):
    head = lax.axis_index("head")
    y, core = head // 2, head % 2
    blocks = ylg_ref.shape[0] // Q
    feat = base_ref.shape[1]
    half = Q // 2
    barrier = pltpu.get_barrier_semaphore()
    for k in range(1, 8):
        pl.semaphore_signal(
            barrier, inc=1, device_id={"head": (head + k) % 8}, device_id_type=MESH
        )

    dests = [(y + 3) % 4, (y + 1) % 4, (y + 2) % 4, y]

    def w_copy(d, side):
        index = d * 2 + side
        at = pl.multiple_of(index * feat, feat)
        return pltpu.make_async_copy(w_ref.at[:, pl.ds(at, feat)], wv.at[index], sem_w.at[index])

    for d in dests:
        for side in (1 - core, core):
            w_copy(d, side).start()

    def pair_copy(b, d):
        return pltpu.make_async_remote_copy(
            src_ref=psend.at[b, d], dst_ref=precv.at[b, d],
            send_sem=sem_ps.at[b, d], recv_sem=sem_pr.at[b, d],
            device_id={"head": y * 2 + 1 - core}, device_id_type=MESH,
        )

    def ring_copy(b, j, way):
        to = (y + 1 + 2 * way) % 4
        return pltpu.make_async_remote_copy(
            src_ref=rsend.at[b, j, way], dst_ref=rrecv.at[b, j, way],
            send_sem=sem_rs.at[b, j, way], recv_sem=sem_rr.at[b, j, way],
            device_id={"head": to * 2 + core}, device_id_type=MESH,
        )

    def low_copy(b):
        return pltpu.make_async_remote_copy(
            src_ref=lsend.at[b], dst_ref=lrecv.at[head],
            send_sem=sem_ls.at[b], recv_sem=sem_lr.at[head],
            device_id={"head": b}, device_id_type=MESH,
        )

    def low_arrival(k):
        return pltpu.make_async_remote_copy(
            src_ref=lsend.at[k], dst_ref=lrecv.at[k],
            send_sem=sem_ls.at[k], recv_sem=sem_lr.at[k],
            device_id={"head": k}, device_id_type=MESH,
        )

    def sum_copy(k):
        return pltpu.make_async_remote_copy(
            src_ref=lout.at[head], dst_ref=lout.at[head],
            send_sem=sem_as.at[k], recv_sem=sem_ar.at[head],
            device_id={"head": k}, device_id_type=MESH,
        )

    def sum_arrival(k):
        return pltpu.make_async_remote_copy(
            src_ref=lout.at[k], dst_ref=lout.at[k],
            send_sem=sem_as.at[k], recv_sem=sem_ar.at[k],
            device_id={"head": k}, device_id_type=MESH,
        )

    pl.semaphore_wait(barrier, 7)

    def compute(b):
        rows = pl.ds(pl.multiple_of(b * Q, Q), Q)
        got = dot(cc_ref[rows, :], inc_ref[...])
        gated = ylg_ref[rows, :].astype(F32) + eg_ref[rows, :].astype(F32) * got
        scale = lax.rsqrt(jnp.mean(gated * gated, axis=1, keepdims=True) + EPSILON)
        normed = (gated * scale * gain_ref[...].astype(F32)).astype(BF16)
        for d in dests:
            @pl.when(b == 0)
            def _():
                w_copy(d, 1 - core).wait()
            psend[b, d] = dot(normed, wv[d * 2 + 1 - core]).astype(BF16)
            pair_copy(b, d).start()

            @pl.when(b == 0)
            def _():
                w_copy(d, core).wait()
            own[b, d] = dot(normed, wv[d * 2 + core])
        low = dot_dims(down_ref[slot_ref[b], :, 0 : ylg_ref.shape[1]], normed, 1, 1).astype(BF16)
        lsend[b] = low

        @pl.when(b == head)
        def _():
            lrecv[b] = low

        @pl.when(b != head)
        def _():
            low_copy(b).start()

    def ring(b, j):
        if j == 0:
            pair_copy(b, dests[0]).wait_recv()
            pair_copy(b, dests[1]).wait_recv()
        elif j == 1:
            pair_copy(b, dests[2]).wait_recv()
        elif j == 3:
            pair_copy(b, dests[3]).wait_recv()
        for way in range(2):
            d = (y + (j + 1) * (3 - 2 * way)) % 4
            part = slice(way * half, way * half + half)
            value = own[b, d, part, :] + precv[b, d, part, :].astype(F32)
            if j > 0:
                ring_copy(b, j - 1, way).wait_recv()
                value = value + rrecv[b, j - 1, way].astype(F32)
            if j < 3:
                rsend[b, j, way] = value.astype(BF16)
                ring_copy(b, j, way).start()
            else:
                at = pl.multiple_of(b * Q + way * half, half)
                base_ref[pl.ds(at, half), :] = value

    def sum_low():
        for k in range(8):
            @pl.when(k != head)
            def _():
                low_arrival(k).wait_recv()
        total = lrecv[0].astype(F32)
        for k in range(1, 8):
            total = total + lrecv[k].astype(F32)
        lout[head] = total.astype(BF16)
        for k in range(8):
            @pl.when(k != head)
            def _():
                sum_copy(k).start()

    def tick(t, carry):
        @pl.when(t < blocks)
        def _():
            compute(t)

        for j in range(4):
            b = t - LAG[j]

            @pl.when(jnp.logical_and(b >= 0, b < blocks))
            def _():
                ring(b, j)

        @pl.when(t == blocks + 1)
        def _():
            sum_low()

        return carry

    lax.fori_loop(0, blocks + LAG[3], tick, 0)

    for k in range(8):
        @pl.when(k != head)
        def _():
            sum_arrival(k).wait_recv()
            low_copy(k).wait_send()
            sum_copy(k).wait_send()
    low_ref[...] = lout[...]

    def drain(b, carry):
        for d in range(4):
            pair_copy(b, d).wait_send()
        for j in range(3):
            for way in range(2):
                ring_copy(b, j, way).wait_send()
        return carry

    lax.fori_loop(0, blocks, drain, 0)


def project(slots, ylg, eg, cc, inc, gain, down, weight):
    tokens, width = ylg.shape
    feat = weight.shape[1] // 8
    rank = down.shape[1]
    blocks = tokens // Q
    vmem = pl.BlockSpec(memory_space=pltpu.VMEM)
    dma = pltpu.SemaphoreType.DMA
    return pl.pallas_call(
        project_kernel,
        in_specs=[pl.BlockSpec(memory_space=pltpu.SMEM)] + [vmem] * 6 + [pl.BlockSpec(memory_space=pl.ANY)],
        out_specs=[vmem, vmem],
        out_shape=[
            jax.ShapeDtypeStruct((tokens, feat), F32),
            jax.ShapeDtypeStruct((blocks, rank, Q), BF16),
        ],
        scratch_shapes=[
            pltpu.VMEM((8, width, feat), BF16),
            pltpu.VMEM((blocks, 4, Q, feat), F32),
            pltpu.VMEM((blocks, 4, Q, feat), BF16),
            pltpu.VMEM((blocks, 4, Q, feat), BF16),
            pltpu.VMEM((blocks, 3, 2, Q // 2, feat), BF16),
            pltpu.VMEM((blocks, 3, 2, Q // 2, feat), BF16),
            pltpu.VMEM((8, rank, Q), BF16),
            pltpu.VMEM((8, rank, Q), BF16),
            pltpu.VMEM((8, rank, Q), BF16),
            dma((8,)), dma((blocks, 4)), dma((blocks, 4)), dma((blocks, 3, 2)), dma((blocks, 3, 2)),
            dma((8,)), dma((8,)), dma((8,)), dma((8,)),
        ],
        compiler_params=pltpu.CompilerParams(
            collective_id=2, has_side_effects=True, vmem_limit_bytes=VMEM_LIMIT
        ),
        name="project",
    )(slots, ylg, eg, cc, inc, gain, down, weight)


def lay_out_kernel(place_ref, down_ref, up_ref, out_ref):
    group, width = out_ref.shape[0], down_ref.shape[2]
    for k in range(group):
        place = place_ref[pl.program_id(0) * group + k]
        here = jnp.logical_and(place >= 0, place < PANEL_DEV)
        index = jnp.clip(place, 0, PANEL_DEV - 1)
        out_ref[k, :, 0:width] = jnp.where(here, down_ref[index], 0)
        out_ref[k, :, width:] = jnp.where(here, up_ref[index], 0)


def lay_out(places, down, up, group=4):
    turns = places.shape[0]
    rank, width = down.shape[1:]
    total = width + up.shape[2]
    return pl.pallas_call(
        lay_out_kernel,
        grid_spec=pltpu.PrefetchScalarGridSpec(
            num_scalar_prefetch=1,
            grid=(turns // group,),
            in_specs=[
                pl.BlockSpec(down.shape, lambda i, s: (0, 0, 0)),
                pl.BlockSpec(up.shape, lambda i, s: (0, 0, 0)),
            ],
            out_specs=pl.BlockSpec((group, rank, total), lambda i, s: (i, 0, 0)),
        ),
        out_shape=jax.ShapeDtypeStruct((turns, rank, total), BF16),
        name="lay_out",
    )(places, down, up)


def adapt_kernel(slot_ref, base_ref, low_ref, up_ref, out_ref):
    out_ref[...] = (base_ref[...] + dot_dims(low_ref[0], up_ref[0], 0, 0)).astype(BF16)


def adapt(slots, base, low, up):
    tokens, feat = base.shape
    rank = low.shape[1]
    return pl.pallas_call(
        adapt_kernel,
        grid_spec=pltpu.PrefetchScalarGridSpec(
            num_scalar_prefetch=1,
            grid=(tokens // Q,),
            in_specs=[
                pl.BlockSpec((Q, feat), lambda i, s: (i, 0)),
                pl.BlockSpec((1, rank, Q), lambda i, s: (i, 0, 0)),
                pl.BlockSpec((1, rank, feat), lambda i, s: (s[i], 0, up.shape[2] // feat - 1)),
            ],
            out_specs=pl.BlockSpec((Q, feat), lambda i, s: (i, 0)),
        ),
        out_shape=jax.ShapeDtypeStruct((tokens, feat), BF16),
        compiler_params=pltpu.CompilerParams(vmem_limit_bytes=16 * 1024 * 1024),
        name="adapt",
    )(slots, base, low, up)


def local(
    input_x_channels,
    input_b_channels,
    input_c_channels,
    input_gate_channels,
    raw_step_sizes,
    log_decay_rate,
    head_skip_coeff,
    x_conv_taps,
    b_conv_taps,
    c_conv_taps,
    gated_norm_gain,
    output_weight,
    adapter_down_panels,
    adapter_up_panels,
    turn_first_token,
    tenant_of_turn,
    tenant_panel_index,
):
    tokens = input_x_channels.shape[0]
    own = lax.axis_index("ctx")
    homes = jnp.take(tenant_panel_index, tenant_of_turn)
    starts = lax.dynamic_slice_in_dim(turn_first_token, TURN_DEV * own, TURN_DEV, 0)
    places = own * tokens + Q * jnp.arange(tokens // Q)
    slots = jnp.sum((places[:, None] >= starts[None, :]).astype(jnp.int32), axis=1)

    offered = lay_out(homes - PANEL_DEV * own, adapter_down_panels.transpose(0, 2, 1), adapter_up_panels)
    count = lax.axis_size("ctx")
    onward = [(i, i + 1) for i in range(count - 1)]
    mine = lax.psum_scatter(offered, "ctx", scatter_dimension=0, tiled=True)
    before = lax.ppermute(mine[TURN_DEV - 1 :], "ctx", onward)
    panels = jnp.concatenate([before, mine], axis=0)

    tails = jnp.concatenate(
        [input_x_channels[tokens - 8 :], input_b_channels[tokens - 8 :], input_c_channels[tokens - 8 :]],
        axis=1,
    )
    halo = lax.ppermute(tails, "ctx", onward)
    ylg, eg, cc, state, decay = local_scan(
        input_x_channels, input_b_channels, input_c_channels, input_gate_channels, raw_step_sizes,
        log_decay_rate, head_skip_coeff, halo, x_conv_taps, b_conv_taps, c_conv_taps,
    )
    inc = exchange(state, decay)
    base, low = project(slots, ylg, eg, cc, inc, gated_norm_gain.reshape(1, -1), panels, output_weight)
    return adapt(slots, base, low, panels)


def solution(mesh):
    in_specs = (
        P("ctx", "head"),
        P("ctx", "head"),
        P("ctx", "head"),
        P("ctx", "head"),
        P("head", "ctx"),
        P("head"),
        P("head"),
        P(None, "head"),
        P(None, "head"),
        P(None, "head"),
        P("head"),
        P("head", None),
        P("ctx", "head", None),
        P("ctx", None, "head"),
        P(),
        P(),
        P(),
    )
    out_specs = P("ctx", "head")
    return jax.shard_map(local, mesh=mesh, in_specs=in_specs, out_specs=out_specs, check_vma=False)
```

```python
import functools

import jax
import jax.numpy as jnp
from jax import lax
from jax.experimental import pallas as pl
from jax.experimental.pallas import tpu as pltpu
from jax.sharding import PartitionSpec as P

P_SIZE = 64
N = 128
Q = 128
TURN_DEV = 2
PANEL_DEV = 6
LOG2E = 1.4426950408889634
EPSILON = 1e-05
VMEM_LIMIT = 60 * 1024 * 1024
MESH = pl.DeviceIdType.MESH
F32 = jnp.float32
BF16 = jnp.bfloat16


def silu(v):
    half = 0.5 * v
    return half + half * jnp.tanh(half)


def dot(a, b):
    return jnp.dot(a, b, preferred_element_type=F32)


def dot_dims(a, b, ca, cb):
    return lax.dot_general(a, b, (((ca,), (cb,)), ((), ())), preferred_element_type=F32)


def scan_kernel(
    rate_ref, skip_ref, x_ref, b_ref, c_ref, z_ref, raw_ref, halo_ref, xt_ref, bt_ref, ct_ref,
    ylg_ref, eg_ref, cc_ref, s_ref, d_ref,
    xp, bp, cp, start, skl,
):
    step = pl.program_id(0)
    heads = raw_ref.shape[0]
    width = x_ref.shape[1]
    lane = lax.broadcasted_iota(jnp.int32, (8, 128), 1)

    @pl.when(step == 0)
    def _():
        xp[0:8, :] = halo_ref[:, 0:width].astype(F32)
        bp[0:8, :] = halo_ref[:, width : width + N].astype(F32)
        cp[0:8, :] = halo_ref[:, width + N : width + 2 * N].astype(F32)
        start[...] = jnp.zeros_like(start)
        s_ref[...] = jnp.zeros_like(s_ref)
        for pair in range(heads // 2):
            skl[:, pair * 128 : pair * 128 + 128] = jnp.where(
                lane < P_SIZE, skip_ref[2 * pair], skip_ref[2 * pair + 1]
            )

    @pl.when(step > 0)
    def _():
        xp[0:8, :] = xp[Q : Q + 8, :]
        bp[0:8, :] = bp[Q : Q + 8, :]
        cp[0:8, :] = cp[Q : Q + 8, :]

    xp[8 : 8 + Q, :] = x_ref[...].astype(F32)
    bp[8 : 8 + Q, :] = b_ref[...].astype(F32)
    cp[8 : 8 + Q, :] = c_ref[...].astype(F32)

    def conv(padded, taps, sl):
        total = taps[0:1, sl].astype(F32) * padded[5 : 5 + Q, sl]
        for k in range(1, 4):
            total = total + taps[k : k + 1, sl].astype(F32) * padded[5 + k : 5 + k + Q, sl]
        return silu(total).astype(BF16)

    every = slice(0, N)
    bc = conv(bp, bt_ref, every)
    cc = conv(cp, ct_ref, every)
    cc_ref[...] = cc
    bt = bc.astype(F32).T.astype(BF16)
    row = lax.broadcasted_iota(jnp.int32, (Q, Q), 0)
    col = lax.broadcasted_iota(jnp.int32, (Q, Q), 1)
    scores = jnp.where(row >= col, dot(cc, bt), 0.0)

    raw = raw_ref[...]
    dt = jnp.maximum(raw, 0.0) + jnp.log1p(jnp.exp(-jnp.abs(raw)))
    hrow = lax.broadcasted_iota(jnp.int32, (heads, Q), 0)
    lrow = lax.broadcasted_iota(jnp.int32, (heads, Q), 1)
    rate = jnp.zeros((heads, Q), F32)
    for h in range(heads):
        rate = jnp.where(hrow == h, rate_ref[h], rate)
    run = -dt * jnp.exp(rate)
    shift = 1
    while shift < Q:
        run = run + jnp.where(lrow >= shift, pltpu.roll(run, shift, 1), 0.0)
        shift *= 2
    run2 = run * LOG2E
    last2 = jnp.broadcast_to(run2[:, Q - 1 : Q], (heads, Q))
    stacked = jnp.concatenate(
        [dt, run2] + [jnp.zeros((heads, Q), F32)] * ((Q - 2 * heads) // heads), axis=0
    )
    tr = stacked.T
    before2 = start[...]
    start[...] = before2 + last2
    half_lane = lax.broadcasted_iota(jnp.int32, (Q, 128), 1) < P_SIZE
    half_row = lax.broadcasted_iota(jnp.int32, (1, 128), 1) < P_SIZE

    for pair in range(heads // 2):
        h0, h1 = 2 * pair, 2 * pair + 1
        sl = slice(pair * 128, pair * 128 + 128)
        xc = conv(xp, xt_ref, sl).astype(F32)
        dt_e = jnp.where(half_lane, tr[:, h0 : h0 + 1], tr[:, h1 : h1 + 1])
        c0 = jnp.broadcast_to(tr[:, heads + h0 : heads + h0 + 1], (Q, Q))
        c1 = jnp.broadcast_to(tr[:, heads + h1 : heads + h1 + 1], (Q, Q))
        run_e = jnp.where(half_lane, c0, c1)
        last_e = jnp.where(half_row, last2[h0 : h0 + 1, :], last2[h1 : h1 + 1, :])
        start_e = jnp.where(half_row, before2[h0 : h0 + 1, :], before2[h1 : h1 + 1, :])
        xdt = xc * dt_e
        m0 = (scores * jnp.exp2(jnp.minimum(c0 - run2[h0 : h0 + 1, :], 0.0))).astype(BF16)
        m1 = (scores * jnp.exp2(jnp.minimum(c1 - run2[h1 : h1 + 1, :], 0.0))).astype(BF16)
        mixing = jnp.concatenate([m0, m1], axis=1)
        xdt_pair = jnp.concatenate(
            [jnp.where(half_lane, xdt, 0.0), jnp.where(half_lane, 0.0, xdt)], axis=0
        ).astype(BF16)
        grow = jnp.exp2(run_e)
        carried = s_ref[:, sl]
        y = dot(mixing, xdt_pair) + grow * dot(cc, carried.astype(BF16)) + skl[0:1, sl] * xc
        gate = silu(z_ref[:, sl].astype(F32))
        ylg_ref[:, sl] = (y * gate).astype(BF16)
        eg_ref[:, sl] = (grow * jnp.exp2(start_e) * gate).astype(BF16)
        weighted = (xdt * jnp.exp2(last_e - run_e)).astype(BF16)
        s_ref[:, sl] = jnp.exp2(last_e) * carried + dot(bt, weighted)
        d_ref[:, sl] = jnp.broadcast_to(jnp.exp2(start_e + last_e), (8, 128))


def local_scan(x, b, c, z, raw, rate, skip, halo, xt, bt, ct):
    tokens, width = x.shape
    heads = raw.shape[0]
    smem = pl.BlockSpec(memory_space=pltpu.SMEM)
    whole = lambda a: pl.BlockSpec(a.shape, lambda i: (0,) * a.ndim)
    rows = lambda w: pl.BlockSpec((Q, w), lambda i: (i, 0))
    return pl.pallas_call(
        scan_kernel,
        grid=(tokens // Q,),
        in_specs=[
            smem, smem, rows(width), rows(N), rows(N), rows(width),
            pl.BlockSpec((heads, Q), lambda i: (0, i)),
            whole(halo), whole(xt), whole(bt), whole(ct),
        ],
        out_specs=[
            rows(width), rows(width), rows(N),
            pl.BlockSpec((N, width), lambda i: (0, 0)),
            pl.BlockSpec((8, width), lambda i: (0, 0)),
        ],
        out_shape=[
            jax.ShapeDtypeStruct((tokens, width), BF16),
            jax.ShapeDtypeStruct((tokens, width), BF16),
            jax.ShapeDtypeStruct((tokens, N), BF16),
            jax.ShapeDtypeStruct((N, width), F32),
            jax.ShapeDtypeStruct((8, width), F32),
        ],
        scratch_shapes=[
            pltpu.VMEM((Q + 8, width), F32),
            pltpu.VMEM((Q + 8, N), F32),
            pltpu.VMEM((Q + 8, N), F32),
            pltpu.VMEM((heads, Q), F32),
            pltpu.VMEM((8, width), F32),
        ],
        compiler_params=pltpu.CompilerParams(
            dimension_semantics=("arbitrary",), vmem_limit_bytes=VMEM_LIMIT
        ),
        name="local_scan",
    )(rate, skip, x, b, c, z, raw, halo, xt, bt, ct)


def partners():
    me = lax.axis_index("ctx")
    x, z = me // 4, me % 4
    return [
        (x * 4 + (z + 1 - 2 * (z % 2)), z % 2),
        (x * 4 + (3 - z), z // 2),
        ((x + 1 - 2 * (x % 2)) * 4 + z, x % 2),
        ((3 - x) * 4 + z, x // 2),
    ]


def exchange_kernel(
    s_ref, d_ref, inc_ref, total, prefix, decay, dsend, drecv, ssend, srecv,
    sem_ds, sem_dr, sem_ss, sem_sr, *, chunks,
):
    steps = partners()
    barrier = pltpu.get_barrier_semaphore()
    for other, _ in steps:
        pl.semaphore_signal(barrier, inc=1, device_id={"ctx": other}, device_id_type=MESH)
    width = s_ref.shape[1]
    cw = width // chunks

    def state_copy(c, s):
        return pltpu.make_async_remote_copy(
            src_ref=ssend.at[s, c], dst_ref=srecv.at[s, c],
            send_sem=sem_ss.at[s, c], recv_sem=sem_sr.at[s, c],
            device_id={"ctx": steps[s][0]}, device_id_type=MESH,
        )

    def decay_copy(s):
        return pltpu.make_async_remote_copy(
            src_ref=dsend.at[s], dst_ref=drecv.at[s],
            send_sem=sem_ds.at[s], recv_sem=sem_dr.at[s],
            device_id={"ctx": steps[s][0]}, device_id_type=MESH,
        )

    for c in range(chunks):
        ssend[0, c] = s_ref[:, c * cw : c * cw + cw].astype(BF16)
    dsend[0] = d_ref[...]
    total[...] = s_ref[...]
    prefix[...] = jnp.zeros_like(prefix)
    pl.semaphore_wait(barrier, len(steps))
    decay_copy(0).start()
    for c in range(chunks):
        state_copy(c, 0).start()
    decay[0] = d_ref[...]
    decay[1] = jnp.ones_like(d_ref)
    for wave in range(chunks + 3):
        for s in range(4):
            c = wave - s
            if c < 0 or c >= chunks:
                continue
            sl = slice(c * cw, c * cw + cw)
            upper = steps[s][1] == 1
            if c == 0:
                decay_copy(s).wait_recv()
                theirs = drecv[s]
                decay[2 * s + 2] = decay[2 * s] * theirs
                decay[2 * s + 3] = decay[2 * s + 1] * jnp.where(upper, theirs, 1.0)
                if s < 3:
                    dsend[s + 1] = decay[2 * s + 2]
                    decay_copy(s + 1).start()
            state_copy(c, s).wait_recv()
            incoming = srecv[s, c].astype(F32)
            mine = decay[2 * s, 0:1, sl]
            ahead = decay[2 * s + 1, 0:1, sl]
            theirs = drecv[s, 0:1, sl]
            prefix[:, sl] = prefix[:, sl] + jnp.where(upper, ahead, 0.0) * incoming
            if s < 3:
                new = (
                    jnp.where(upper, mine, 1.0) * incoming
                    + jnp.where(upper, 1.0, theirs) * total[:, sl]
                )
                total[:, sl] = new
                ssend[s + 1, c] = new.astype(BF16)
                state_copy(c, s + 1).start()
    inc_ref[...] = prefix[...].astype(BF16)
    for s in range(4):
        decay_copy(s).wait_send()
        for c in range(chunks):
            state_copy(c, s).wait_send()


def exchange(state, decay, chunks=8):
    width = state.shape[1]
    cw = width // chunks
    vmem = pl.BlockSpec(memory_space=pltpu.VMEM)
    return pl.pallas_call(
        functools.partial(exchange_kernel, chunks=chunks),
        in_specs=[vmem, vmem],
        out_specs=vmem,
        out_shape=jax.ShapeDtypeStruct((N, width), BF16),
        scratch_shapes=[
            pltpu.VMEM((N, width), F32),
            pltpu.VMEM((N, width), F32),
            pltpu.VMEM((10, 8, width), F32),
            pltpu.VMEM((4, 8, width), F32),
            pltpu.VMEM((4, 8, width), F32),
            pltpu.VMEM((4, chunks, N, cw), BF16),
            pltpu.VMEM((4, chunks, N, cw), BF16),
            pltpu.SemaphoreType.DMA((4,)),
            pltpu.SemaphoreType.DMA((4,)),
            pltpu.SemaphoreType.DMA((4, chunks)),
            pltpu.SemaphoreType.DMA((4, chunks)),
        ],
        compiler_params=pltpu.CompilerParams(
            collective_id=1, has_side_effects=True, vmem_limit_bytes=VMEM_LIMIT
        ),
        name="state_exchange",
    )(state, decay)


LAG = (1, 2, 3, 4)


def project_kernel(
    slot_ref, ylg_ref, eg_ref, cc_ref, inc_ref, gain_ref, down_ref, w_ref,
    base_ref, low_ref,
    wv, own, psend, precv, rsend, rrecv, lsend, lrecv, lout,
    sem_w, sem_ps, sem_pr, sem_rs, sem_rr, sem_ls, sem_lr, sem_as, sem_ar,
):
    head = lax.axis_index("head")
    y, core = head // 2, head % 2
    blocks = ylg_ref.shape[0] // Q
    feat = base_ref.shape[1]
    half = Q // 2
    barrier = pltpu.get_barrier_semaphore()
    for k in range(1, 8):
        pl.semaphore_signal(
            barrier, inc=1, device_id={"head": (head + k) % 8}, device_id_type=MESH
        )

    dests = [(y + 3) % 4, (y + 1) % 4, (y + 2) % 4, y]

    def w_copy(d, side):
        index = d * 2 + side
        at = pl.multiple_of(index * feat, feat)
        return pltpu.make_async_copy(w_ref.at[:, pl.ds(at, feat)], wv.at[index], sem_w.at[index])

    for d in dests:
        for side in (1 - core, core):
            w_copy(d, side).start()

    def pair_copy(b, d):
        return pltpu.make_async_remote_copy(
            src_ref=psend.at[b, d], dst_ref=precv.at[b, d],
            send_sem=sem_ps.at[b, d], recv_sem=sem_pr.at[b, d],
            device_id={"head": y * 2 + 1 - core}, device_id_type=MESH,
        )

    def ring_copy(b, j, way):
        to = (y + 1 + 2 * way) % 4
        return pltpu.make_async_remote_copy(
            src_ref=rsend.at[b, j, way], dst_ref=rrecv.at[b, j, way],
            send_sem=sem_rs.at[b, j, way], recv_sem=sem_rr.at[b, j, way],
            device_id={"head": to * 2 + core}, device_id_type=MESH,
        )

    def low_copy(b):
        return pltpu.make_async_remote_copy(
            src_ref=lsend.at[b], dst_ref=lrecv.at[head],
            send_sem=sem_ls.at[b], recv_sem=sem_lr.at[head],
            device_id={"head": b}, device_id_type=MESH,
        )

    def low_arrival(k):
        return pltpu.make_async_remote_copy(
            src_ref=lsend.at[k], dst_ref=lrecv.at[k],
            send_sem=sem_ls.at[k], recv_sem=sem_lr.at[k],
            device_id={"head": k}, device_id_type=MESH,
        )

    def sum_copy(k):
        return pltpu.make_async_remote_copy(
            src_ref=lout.at[head], dst_ref=lout.at[head],
            send_sem=sem_as.at[k], recv_sem=sem_ar.at[head],
            device_id={"head": k}, device_id_type=MESH,
        )

    def sum_arrival(k):
        return pltpu.make_async_remote_copy(
            src_ref=lout.at[k], dst_ref=lout.at[k],
            send_sem=sem_as.at[k], recv_sem=sem_ar.at[k],
            device_id={"head": k}, device_id_type=MESH,
        )

    pl.semaphore_wait(barrier, 7)

    def compute(b):
        rows = pl.ds(pl.multiple_of(b * Q, Q), Q)
        got = dot(cc_ref[rows, :], inc_ref[...])
        gated = ylg_ref[rows, :].astype(F32) + eg_ref[rows, :].astype(F32) * got
        scale = lax.rsqrt(jnp.mean(gated * gated, axis=1, keepdims=True) + EPSILON)
        normed = (gated * scale * gain_ref[...].astype(F32)).astype(BF16)
        for d in dests:
            @pl.when(b == 0)
            def _():
                w_copy(d, 1 - core).wait()
            psend[b, d] = dot(normed, wv[d * 2 + 1 - core]).astype(BF16)
            pair_copy(b, d).start()

            @pl.when(b == 0)
            def _():
                w_copy(d, core).wait()
            own[b, d] = dot(normed, wv[d * 2 + core])
        low = dot_dims(down_ref[slot_ref[b], :, 0 : ylg_ref.shape[1]], normed, 1, 1).astype(BF16)
        lsend[b] = low

        @pl.when(b == head)
        def _():
            lrecv[b] = low

        @pl.when(b != head)
        def _():
            low_copy(b).start()

    def ring(b, j):
        if j == 0:
            pair_copy(b, dests[0]).wait_recv()
            pair_copy(b, dests[1]).wait_recv()
        elif j == 1:
            pair_copy(b, dests[2]).wait_recv()
        elif j == 3:
            pair_copy(b, dests[3]).wait_recv()
        for way in range(2):
            d = (y + (j + 1) * (3 - 2 * way)) % 4
            part = slice(way * half, way * half + half)
            value = own[b, d, part, :] + precv[b, d, part, :].astype(F32)
            if j > 0:
                ring_copy(b, j - 1, way).wait_recv()
                value = value + rrecv[b, j - 1, way].astype(F32)
            if j < 3:
                rsend[b, j, way] = value.astype(BF16)
                ring_copy(b, j, way).start()
            else:
                at = pl.multiple_of(b * Q + way * half, half)
                base_ref[pl.ds(at, half), :] = value

    def sum_low():
        for k in range(8):
            @pl.when(k != head)
            def _():
                low_arrival(k).wait_recv()
        total = lrecv[0].astype(F32)
        for k in range(1, 8):
            total = total + lrecv[k].astype(F32)
        lout[head] = total.astype(BF16)
        for k in range(8):
            @pl.when(k != head)
            def _():
                sum_copy(k).start()

    def tick(t, carry):
        @pl.when(t < blocks)
        def _():
            compute(t)

        for j in range(4):
            b = t - LAG[j]

            @pl.when(jnp.logical_and(b >= 0, b < blocks))
            def _():
                ring(b, j)

        @pl.when(t == blocks + 1)
        def _():
            sum_low()

        return carry

    lax.fori_loop(0, blocks + LAG[3], tick, 0)

    for k in range(8):
        @pl.when(k != head)
        def _():
            sum_arrival(k).wait_recv()
            low_copy(k).wait_send()
            sum_copy(k).wait_send()
    low_ref[...] = lout[...]

    def drain(b, carry):
        for d in range(4):
            pair_copy(b, d).wait_send()
        for j in range(3):
            for way in range(2):
                ring_copy(b, j, way).wait_send()
        return carry

    lax.fori_loop(0, blocks, drain, 0)


def project(slots, ylg, eg, cc, inc, gain, down, weight):
    tokens, width = ylg.shape
    feat = weight.shape[1] // 8
    rank = down.shape[1]
    blocks = tokens // Q
    vmem = pl.BlockSpec(memory_space=pltpu.VMEM)
    dma = pltpu.SemaphoreType.DMA
    return pl.pallas_call(
        project_kernel,
        in_specs=[pl.BlockSpec(memory_space=pltpu.SMEM)] + [vmem] * 6 + [pl.BlockSpec(memory_space=pl.ANY)],
        out_specs=[vmem, vmem],
        out_shape=[
            jax.ShapeDtypeStruct((tokens, feat), F32),
            jax.ShapeDtypeStruct((blocks, rank, Q), BF16),
        ],
        scratch_shapes=[
            pltpu.VMEM((8, width, feat), BF16),
            pltpu.VMEM((blocks, 4, Q, feat), F32),
            pltpu.VMEM((blocks, 4, Q, feat), BF16),
            pltpu.VMEM((blocks, 4, Q, feat), BF16),
            pltpu.VMEM((blocks, 3, 2, Q // 2, feat), BF16),
            pltpu.VMEM((blocks, 3, 2, Q // 2, feat), BF16),
            pltpu.VMEM((8, rank, Q), BF16),
            pltpu.VMEM((8, rank, Q), BF16),
            pltpu.VMEM((8, rank, Q), BF16),
            dma((8,)), dma((blocks, 4)), dma((blocks, 4)), dma((blocks, 3, 2)), dma((blocks, 3, 2)),
            dma((8,)), dma((8,)), dma((8,)), dma((8,)),
        ],
        compiler_params=pltpu.CompilerParams(
            collective_id=2, has_side_effects=True, vmem_limit_bytes=VMEM_LIMIT
        ),
        name="project",
    )(slots, ylg, eg, cc, inc, gain, down, weight)


def lay_out_kernel(place_ref, down_ref, up_ref, out_ref):
    group, width = out_ref.shape[0], down_ref.shape[2]
    for k in range(group):
        place = place_ref[pl.program_id(0) * group + k]
        here = jnp.logical_and(place >= 0, place < PANEL_DEV)
        index = jnp.clip(place, 0, PANEL_DEV - 1)
        out_ref[k, :, 0:width] = jnp.where(here, down_ref[index], 0)
        out_ref[k, :, width:] = jnp.where(here, up_ref[index], 0)


def lay_out(places, down, up, group=4):
    turns = places.shape[0]
    rank, width = down.shape[1:]
    total = width + up.shape[2]
    return pl.pallas_call(
        lay_out_kernel,
        grid_spec=pltpu.PrefetchScalarGridSpec(
            num_scalar_prefetch=1,
            grid=(turns // group,),
            in_specs=[
                pl.BlockSpec(down.shape, lambda i, s: (0, 0, 0)),
                pl.BlockSpec(up.shape, lambda i, s: (0, 0, 0)),
            ],
            out_specs=pl.BlockSpec((group, rank, total), lambda i, s: (i, 0, 0)),
        ),
        out_shape=jax.ShapeDtypeStruct((turns, rank, total), BF16),
        name="lay_out",
    )(places, down, up)


def adapt_kernel(slot_ref, base_ref, low_ref, up_ref, out_ref):
    out_ref[...] = (base_ref[...] + dot_dims(low_ref[0], up_ref[0], 0, 0)).astype(BF16)


def adapt(slots, base, low, up):
    tokens, feat = base.shape
    rank = low.shape[1]
    return pl.pallas_call(
        adapt_kernel,
        grid_spec=pltpu.PrefetchScalarGridSpec(
            num_scalar_prefetch=1,
            grid=(tokens // Q,),
            in_specs=[
                pl.BlockSpec((Q, feat), lambda i, s: (i, 0)),
                pl.BlockSpec((1, rank, Q), lambda i, s: (i, 0, 0)),
                pl.BlockSpec((1, rank, feat), lambda i, s: (s[i], 0, up.shape[2] // feat - 1)),
            ],
            out_specs=pl.BlockSpec((Q, feat), lambda i, s: (i, 0)),
        ),
        out_shape=jax.ShapeDtypeStruct((tokens, feat), BF16),
        compiler_params=pltpu.CompilerParams(vmem_limit_bytes=16 * 1024 * 1024),
        name="adapt",
    )(slots, base, low, up)


def local(
    input_x_channels,
    input_b_channels,
    input_c_channels,
    input_gate_channels,
    raw_step_sizes,
    log_decay_rate,
    head_skip_coeff,
    x_conv_taps,
    b_conv_taps,
    c_conv_taps,
    gated_norm_gain,
    output_weight,
    adapter_down_panels,
    adapter_up_panels,
    turn_first_token,
    tenant_of_turn,
    tenant_panel_index,
):
    tokens = input_x_channels.shape[0]
    own = lax.axis_index("ctx")
    homes = jnp.take(tenant_panel_index, tenant_of_turn)
    starts = lax.dynamic_slice_in_dim(turn_first_token, TURN_DEV * own, TURN_DEV, 0)
    places = own * tokens + Q * jnp.arange(tokens // Q)
    slots = jnp.sum((places[:, None] >= starts[None, :]).astype(jnp.int32), axis=1)

    offered = lay_out(homes - PANEL_DEV * own, adapter_down_panels.transpose(0, 2, 1), adapter_up_panels)
    count = lax.axis_size("ctx")
    onward = [(i, i + 1) for i in range(count - 1)]
    mine = lax.psum_scatter(offered, "ctx", scatter_dimension=0, tiled=True)

    tails = jnp.concatenate(
        [input_x_channels[tokens - 8 :], input_b_channels[tokens - 8 :], input_c_channels[tokens - 8 :]],
        axis=1,
    )
    halo = lax.ppermute(tails, "ctx", onward)
    ylg, eg, cc, state, decay = local_scan(
        input_x_channels, input_b_channels, input_c_channels, input_gate_channels, raw_step_sizes,
        log_decay_rate, head_skip_coeff, halo, x_conv_taps, b_conv_taps, c_conv_taps,
    )
    inc = exchange(state, decay)
    mine, inc = lax.optimization_barrier((mine, inc))
    before = lax.ppermute(mine[TURN_DEV - 1 :], "ctx", onward)
    panels = jnp.concatenate([before, mine], axis=0)
    base, low = project(slots, ylg, eg, cc, inc, gated_norm_gain.reshape(1, -1), panels, output_weight)
    return adapt(slots, base, low, panels)


def solution(mesh):
    in_specs = (
        P("ctx", "head"),
        P("ctx", "head"),
        P("ctx", "head"),
        P("ctx", "head"),
        P("head", "ctx"),
        P("head"),
        P("head"),
        P(None, "head"),
        P(None, "head"),
        P(None, "head"),
        P("head"),
        P("head", None),
        P("ctx", "head", None),
        P("ctx", None, "head"),
        P(),
        P(),
        P(),
    )
    out_specs = P("ctx", "head")
    return jax.shard_map(local, mesh=mesh, in_specs=in_specs, out_specs=out_specs, check_vma=False)
```

```python
import functools

import jax
import jax.numpy as jnp
from jax import lax
from jax.experimental import pallas as pl
from jax.experimental.pallas import tpu as pltpu
from jax.sharding import PartitionSpec as P

P_SIZE = 64
N = 128
Q = 128
TURN_DEV = 2
PANEL_DEV = 6
WAVE_LAG = 3
LOG2E = 1.4426950408889634
EPSILON = 1e-05
VMEM_LIMIT = 60 * 1024 * 1024
MESH = pl.DeviceIdType.MESH
F32 = jnp.float32
BF16 = jnp.bfloat16


def silu(v):
    half = 0.5 * v
    return half + half * jnp.tanh(half)


def dot(a, b):
    return jnp.dot(a, b, preferred_element_type=F32)


def dot_dims(a, b, ca, cb):
    return lax.dot_general(a, b, (((ca,), (cb,)), ((), ())), preferred_element_type=F32)


def scan_kernel(
    rate_ref, skip_ref, x_ref, b_ref, c_ref, z_ref, raw_ref, halo_ref, xt_ref, bt_ref, ct_ref,
    ylg_ref, eg_ref, cc_ref, s_ref, d_ref,
    xp, bp, cp, start, skl,
):
    step = pl.program_id(0)
    heads = raw_ref.shape[0]
    width = x_ref.shape[1]
    lane = lax.broadcasted_iota(jnp.int32, (8, 128), 1)

    @pl.when(step == 0)
    def _():
        xp[0:8, :] = halo_ref[:, 0:width].astype(F32)
        bp[0:8, :] = halo_ref[:, width : width + N].astype(F32)
        cp[0:8, :] = halo_ref[:, width + N : width + 2 * N].astype(F32)
        start[...] = jnp.zeros_like(start)
        s_ref[...] = jnp.zeros_like(s_ref)
        for pair in range(heads // 2):
            skl[:, pair * 128 : pair * 128 + 128] = jnp.where(
                lane < P_SIZE, skip_ref[2 * pair], skip_ref[2 * pair + 1]
            )

    @pl.when(step > 0)
    def _():
        xp[0:8, :] = xp[Q : Q + 8, :]
        bp[0:8, :] = bp[Q : Q + 8, :]
        cp[0:8, :] = cp[Q : Q + 8, :]

    xp[8 : 8 + Q, :] = x_ref[...].astype(F32)
    bp[8 : 8 + Q, :] = b_ref[...].astype(F32)
    cp[8 : 8 + Q, :] = c_ref[...].astype(F32)

    def conv(padded, taps, sl):
        total = taps[0:1, sl].astype(F32) * padded[5 : 5 + Q, sl]
        for k in range(1, 4):
            total = total + taps[k : k + 1, sl].astype(F32) * padded[5 + k : 5 + k + Q, sl]
        return silu(total).astype(BF16)

    every = slice(0, N)
    bc = conv(bp, bt_ref, every)
    cc = conv(cp, ct_ref, every)
    cc_ref[...] = cc
    bt = bc.astype(F32).T.astype(BF16)
    row = lax.broadcasted_iota(jnp.int32, (Q, Q), 0)
    col = lax.broadcasted_iota(jnp.int32, (Q, Q), 1)
    scores = jnp.where(row >= col, dot(cc, bt), 0.0)

    raw = raw_ref[...]
    dt = jnp.maximum(raw, 0.0) + jnp.log1p(jnp.exp(-jnp.abs(raw)))
    hrow = lax.broadcasted_iota(jnp.int32, (heads, Q), 0)
    lrow = lax.broadcasted_iota(jnp.int32, (heads, Q), 1)
    rate = jnp.zeros((heads, Q), F32)
    for h in range(heads):
        rate = jnp.where(hrow == h, rate_ref[h], rate)
    run = -dt * jnp.exp(rate)
    shift = 1
    while shift < Q:
        run = run + jnp.where(lrow >= shift, pltpu.roll(run, shift, 1), 0.0)
        shift *= 2
    run2 = run * LOG2E
    last2 = jnp.broadcast_to(run2[:, Q - 1 : Q], (heads, Q))
    stacked = jnp.concatenate(
        [dt, run2] + [jnp.zeros((heads, Q), F32)] * ((Q - 2 * heads) // heads), axis=0
    )
    tr = stacked.T
    before2 = start[...]
    start[...] = before2 + last2
    half_lane = lax.broadcasted_iota(jnp.int32, (Q, 128), 1) < P_SIZE
    half_row = lax.broadcasted_iota(jnp.int32, (1, 128), 1) < P_SIZE

    for pair in range(heads // 2):
        h0, h1 = 2 * pair, 2 * pair + 1
        sl = slice(pair * 128, pair * 128 + 128)
        xc = conv(xp, xt_ref, sl).astype(F32)
        dt_e = jnp.where(half_lane, tr[:, h0 : h0 + 1], tr[:, h1 : h1 + 1])
        c0 = jnp.broadcast_to(tr[:, heads + h0 : heads + h0 + 1], (Q, Q))
        c1 = jnp.broadcast_to(tr[:, heads + h1 : heads + h1 + 1], (Q, Q))
        run_e = jnp.where(half_lane, c0, c1)
        last_e = jnp.where(half_row, last2[h0 : h0 + 1, :], last2[h1 : h1 + 1, :])
        start_e = jnp.where(half_row, before2[h0 : h0 + 1, :], before2[h1 : h1 + 1, :])
        xdt = xc * dt_e
        m0 = (scores * jnp.exp2(jnp.minimum(c0 - run2[h0 : h0 + 1, :], 0.0))).astype(BF16)
        m1 = (scores * jnp.exp2(jnp.minimum(c1 - run2[h1 : h1 + 1, :], 0.0))).astype(BF16)
        mixing = jnp.concatenate([m0, m1], axis=1)
        xdt_pair = jnp.concatenate(
            [jnp.where(half_lane, xdt, 0.0), jnp.where(half_lane, 0.0, xdt)], axis=0
        ).astype(BF16)
        grow = jnp.exp2(run_e)
        carried = s_ref[:, sl]
        y = dot(mixing, xdt_pair) + grow * dot(cc, carried.astype(BF16)) + skl[0:1, sl] * xc
        gate = silu(z_ref[:, sl].astype(F32))
        ylg_ref[:, sl] = (y * gate).astype(BF16)
        eg_ref[:, sl] = (grow * jnp.exp2(start_e) * gate).astype(BF16)
        weighted = (xdt * jnp.exp2(last_e - run_e)).astype(BF16)
        s_ref[:, sl] = jnp.exp2(last_e) * carried + dot(bt, weighted)
        d_ref[:, sl] = jnp.broadcast_to(jnp.exp2(start_e + last_e), (8, 128))


def local_scan(x, b, c, z, raw, rate, skip, halo, xt, bt, ct):
    tokens, width = x.shape
    heads = raw.shape[0]
    smem = pl.BlockSpec(memory_space=pltpu.SMEM)
    whole = lambda a: pl.BlockSpec(a.shape, lambda i: (0,) * a.ndim)
    rows = lambda w: pl.BlockSpec((Q, w), lambda i: (i, 0))
    return pl.pallas_call(
        scan_kernel,
        grid=(tokens // Q,),
        in_specs=[
            smem, smem, rows(width), rows(N), rows(N), rows(width),
            pl.BlockSpec((heads, Q), lambda i: (0, i)),
            whole(halo), whole(xt), whole(bt), whole(ct),
        ],
        out_specs=[
            rows(width), rows(width), rows(N),
            pl.BlockSpec((N, width), lambda i: (0, 0)),
            pl.BlockSpec((8, width), lambda i: (0, 0)),
        ],
        out_shape=[
            jax.ShapeDtypeStruct((tokens, width), BF16),
            jax.ShapeDtypeStruct((tokens, width), BF16),
            jax.ShapeDtypeStruct((tokens, N), BF16),
            jax.ShapeDtypeStruct((N, width), F32),
            jax.ShapeDtypeStruct((8, width), F32),
        ],
        scratch_shapes=[
            pltpu.VMEM((Q + 8, width), F32),
            pltpu.VMEM((Q + 8, N), F32),
            pltpu.VMEM((Q + 8, N), F32),
            pltpu.VMEM((heads, Q), F32),
            pltpu.VMEM((8, width), F32),
        ],
        compiler_params=pltpu.CompilerParams(
            dimension_semantics=("arbitrary",), vmem_limit_bytes=VMEM_LIMIT
        ),
        name="local_scan",
    )(rate, skip, x, b, c, z, raw, halo, xt, bt, ct)


def partners():
    me = lax.axis_index("ctx")
    x, z = me // 4, me % 4
    return [
        (x * 4 + (z + 1 - 2 * (z % 2)), z % 2),
        (x * 4 + (3 - z), z // 2),
        ((x + 1 - 2 * (x % 2)) * 4 + z, x % 2),
        ((3 - x) * 4 + z, x // 2),
    ]


def exchange_kernel(
    s_ref, d_ref, inc_ref, total, prefix, decay, dsend, drecv, ssend, srecv,
    sem_ds, sem_dr, sem_ss, sem_sr, *, chunks,
):
    steps = partners()
    barrier = pltpu.get_barrier_semaphore()
    for other, _ in steps:
        pl.semaphore_signal(barrier, inc=1, device_id={"ctx": other}, device_id_type=MESH)
    width = s_ref.shape[1]
    cw = width // chunks

    def state_copy(c, s):
        return pltpu.make_async_remote_copy(
            src_ref=ssend.at[s, c], dst_ref=srecv.at[s, c],
            send_sem=sem_ss.at[s, c], recv_sem=sem_sr.at[s, c],
            device_id={"ctx": steps[s][0]}, device_id_type=MESH,
        )

    def decay_copy(s):
        return pltpu.make_async_remote_copy(
            src_ref=dsend.at[s], dst_ref=drecv.at[s],
            send_sem=sem_ds.at[s], recv_sem=sem_dr.at[s],
            device_id={"ctx": steps[s][0]}, device_id_type=MESH,
        )

    for c in range(chunks):
        ssend[0, c] = s_ref[:, c * cw : c * cw + cw].astype(BF16)
    dsend[0] = d_ref[...]
    total[...] = s_ref[...]
    prefix[...] = jnp.zeros_like(prefix)
    pl.semaphore_wait(barrier, len(steps))
    decay_copy(0).start()
    for c in range(chunks):
        state_copy(c, 0).start()
    decay[0] = d_ref[...]
    decay[1] = jnp.ones_like(d_ref)
    for wave in range(chunks + 3 * WAVE_LAG):
        for s in range(4):
            c = wave - WAVE_LAG * s
            if c < 0 or c >= chunks:
                continue
            sl = slice(c * cw, c * cw + cw)
            upper = steps[s][1] == 1
            if c == 0:
                decay_copy(s).wait_recv()
                theirs = drecv[s]
                decay[2 * s + 2] = decay[2 * s] * theirs
                decay[2 * s + 3] = decay[2 * s + 1] * jnp.where(upper, theirs, 1.0)
                if s < 3:
                    dsend[s + 1] = decay[2 * s + 2]
                    decay_copy(s + 1).start()
            state_copy(c, s).wait_recv()
            incoming = srecv[s, c].astype(F32)
            mine = decay[2 * s, 0:1, sl]
            ahead = decay[2 * s + 1, 0:1, sl]
            theirs = drecv[s, 0:1, sl]
            prefix[:, sl] = prefix[:, sl] + jnp.where(upper, ahead, 0.0) * incoming
            if s < 3:
                new = (
                    jnp.where(upper, mine, 1.0) * incoming
                    + jnp.where(upper, 1.0, theirs) * total[:, sl]
                )
                total[:, sl] = new
                ssend[s + 1, c] = new.astype(BF16)
                state_copy(c, s + 1).start()
    inc_ref[...] = prefix[...].astype(BF16)
    for s in range(4):
        decay_copy(s).wait_send()
        for c in range(chunks):
            state_copy(c, s).wait_send()


def exchange(state, decay, chunks=8):
    width = state.shape[1]
    cw = width // chunks
    vmem = pl.BlockSpec(memory_space=pltpu.VMEM)
    return pl.pallas_call(
        functools.partial(exchange_kernel, chunks=chunks),
        in_specs=[vmem, vmem],
        out_specs=vmem,
        out_shape=jax.ShapeDtypeStruct((N, width), BF16),
        scratch_shapes=[
            pltpu.VMEM((N, width), F32),
            pltpu.VMEM((N, width), F32),
            pltpu.VMEM((10, 8, width), F32),
            pltpu.VMEM((4, 8, width), F32),
            pltpu.VMEM((4, 8, width), F32),
            pltpu.VMEM((4, chunks, N, cw), BF16),
            pltpu.VMEM((4, chunks, N, cw), BF16),
            pltpu.SemaphoreType.DMA((4,)),
            pltpu.SemaphoreType.DMA((4,)),
            pltpu.SemaphoreType.DMA((4, chunks)),
            pltpu.SemaphoreType.DMA((4, chunks)),
        ],
        compiler_params=pltpu.CompilerParams(
            collective_id=1, has_side_effects=True, vmem_limit_bytes=VMEM_LIMIT
        ),
        name="state_exchange",
    )(state, decay)


LAG = (1, 2, 3, 4)


def project_kernel(
    slot_ref, ylg_ref, eg_ref, cc_ref, inc_ref, gain_ref, down_ref, w_ref,
    base_ref, low_ref,
    wv, own, psend, precv, rsend, rrecv, lsend, lrecv, lout,
    sem_w, sem_ps, sem_pr, sem_rs, sem_rr, sem_ls, sem_lr, sem_as, sem_ar,
):
    head = lax.axis_index("head")
    y, core = head // 2, head % 2
    blocks = ylg_ref.shape[0] // Q
    feat = base_ref.shape[1]
    half = Q // 2
    barrier = pltpu.get_barrier_semaphore()
    for k in range(1, 8):
        pl.semaphore_signal(
            barrier, inc=1, device_id={"head": (head + k) % 8}, device_id_type=MESH
        )

    dests = [(y + 3) % 4, (y + 1) % 4, (y + 2) % 4, y]

    def w_copy(d, side):
        index = d * 2 + side
        at = pl.multiple_of(index * feat, feat)
        return pltpu.make_async_copy(w_ref.at[:, pl.ds(at, feat)], wv.at[index], sem_w.at[index])

    for d in dests:
        for side in (1 - core, core):
            w_copy(d, side).start()

    def pair_copy(b, d):
        return pltpu.make_async_remote_copy(
            src_ref=psend.at[b, d], dst_ref=precv.at[b, d],
            send_sem=sem_ps.at[b, d], recv_sem=sem_pr.at[b, d],
            device_id={"head": y * 2 + 1 - core}, device_id_type=MESH,
        )

    def ring_copy(b, j, way):
        to = (y + 1 + 2 * way) % 4
        return pltpu.make_async_remote_copy(
            src_ref=rsend.at[b, j, way], dst_ref=rrecv.at[b, j, way],
            send_sem=sem_rs.at[b, j, way], recv_sem=sem_rr.at[b, j, way],
            device_id={"head": to * 2 + core}, device_id_type=MESH,
        )

    def low_copy(b):
        return pltpu.make_async_remote_copy(
            src_ref=lsend.at[b], dst_ref=lrecv.at[head],
            send_sem=sem_ls.at[b], recv_sem=sem_lr.at[head],
            device_id={"head": b}, device_id_type=MESH,
        )

    def low_arrival(k):
        return pltpu.make_async_remote_copy(
            src_ref=lsend.at[k], dst_ref=lrecv.at[k],
            send_sem=sem_ls.at[k], recv_sem=sem_lr.at[k],
            device_id={"head": k}, device_id_type=MESH,
        )

    def sum_copy(k):
        return pltpu.make_async_remote_copy(
            src_ref=lout.at[head], dst_ref=lout.at[head],
            send_sem=sem_as.at[k], recv_sem=sem_ar.at[head],
            device_id={"head": k}, device_id_type=MESH,
        )

    def sum_arrival(k):
        return pltpu.make_async_remote_copy(
            src_ref=lout.at[k], dst_ref=lout.at[k],
            send_sem=sem_as.at[k], recv_sem=sem_ar.at[k],
            device_id={"head": k}, device_id_type=MESH,
        )

    pl.semaphore_wait(barrier, 7)

    def compute(b):
        rows = pl.ds(pl.multiple_of(b * Q, Q), Q)
        got = dot(cc_ref[rows, :], inc_ref[...])
        gated = ylg_ref[rows, :].astype(F32) + eg_ref[rows, :].astype(F32) * got
        scale = lax.rsqrt(jnp.mean(gated * gated, axis=1, keepdims=True) + EPSILON)
        normed = (gated * scale * gain_ref[...].astype(F32)).astype(BF16)
        for d in dests:
            @pl.when(b == 0)
            def _():
                w_copy(d, 1 - core).wait()
            psend[b, d] = dot(normed, wv[d * 2 + 1 - core]).astype(BF16)
            pair_copy(b, d).start()

            @pl.when(b == 0)
            def _():
                w_copy(d, core).wait()
            own[b, d] = dot(normed, wv[d * 2 + core])
        low = dot_dims(down_ref[slot_ref[b]], normed, 1, 1).astype(BF16)
        lsend[b] = low

        @pl.when(b == head)
        def _():
            lrecv[b] = low

        @pl.when(b != head)
        def _():
            low_copy(b).start()

    def ring(b, j):
        if j == 0:
            pair_copy(b, dests[0]).wait_recv()
            pair_copy(b, dests[1]).wait_recv()
        elif j == 1:
            pair_copy(b, dests[2]).wait_recv()
        elif j == 3:
            pair_copy(b, dests[3]).wait_recv()
        for way in range(2):
            d = (y + (j + 1) * (3 - 2 * way)) % 4
            part = slice(way * half, way * half + half)
            value = own[b, d, part, :] + precv[b, d, part, :].astype(F32)
            if j > 0:
                ring_copy(b, j - 1, way).wait_recv()
                value = value + rrecv[b, j - 1, way].astype(F32)
            if j < 3:
                rsend[b, j, way] = value.astype(BF16)
                ring_copy(b, j, way).start()
            else:
                at = pl.multiple_of(b * Q + way * half, half)
                base_ref[pl.ds(at, half), :] = value

    def sum_low():
        for k in range(8):
            @pl.when(k != head)
            def _():
                low_arrival(k).wait_recv()
        total = lrecv[0].astype(F32)
        for k in range(1, 8):
            total = total + lrecv[k].astype(F32)
        lout[head] = total.astype(BF16)
        for k in range(8):
            @pl.when(k != head)
            def _():
                sum_copy(k).start()

    def tick(t, carry):
        @pl.when(t < blocks)
        def _():
            compute(t)

        for j in range(4):
            b = t - LAG[j]

            @pl.when(jnp.logical_and(b >= 0, b < blocks))
            def _():
                ring(b, j)

        @pl.when(t == blocks + 1)
        def _():
            sum_low()

        return carry

    lax.fori_loop(0, blocks + LAG[3], tick, 0)

    for k in range(8):
        @pl.when(k != head)
        def _():
            sum_arrival(k).wait_recv()
            low_copy(k).wait_send()
            sum_copy(k).wait_send()
    low_ref[...] = lout[...]

    def drain(b, carry):
        for d in range(4):
            pair_copy(b, d).wait_send()
        for j in range(3):
            for way in range(2):
                ring_copy(b, j, way).wait_send()
        return carry

    lax.fori_loop(0, blocks, drain, 0)


def project(slots, ylg, eg, cc, inc, gain, down, weight):
    tokens, width = ylg.shape
    feat = weight.shape[1] // 8
    rank = down.shape[1]
    blocks = tokens // Q
    vmem = pl.BlockSpec(memory_space=pltpu.VMEM)
    dma = pltpu.SemaphoreType.DMA
    return pl.pallas_call(
        project_kernel,
        in_specs=[pl.BlockSpec(memory_space=pltpu.SMEM)] + [vmem] * 6 + [pl.BlockSpec(memory_space=pl.ANY)],
        out_specs=[vmem, vmem],
        out_shape=[
            jax.ShapeDtypeStruct((tokens, feat), F32),
            jax.ShapeDtypeStruct((blocks, rank, Q), BF16),
        ],
        scratch_shapes=[
            pltpu.VMEM((8, width, feat), BF16),
            pltpu.VMEM((blocks, 4, Q, feat), F32),
            pltpu.VMEM((blocks, 4, Q, feat), BF16),
            pltpu.VMEM((blocks, 4, Q, feat), BF16),
            pltpu.VMEM((blocks, 3, 2, Q // 2, feat), BF16),
            pltpu.VMEM((blocks, 3, 2, Q // 2, feat), BF16),
            pltpu.VMEM((8, rank, Q), BF16),
            pltpu.VMEM((8, rank, Q), BF16),
            pltpu.VMEM((8, rank, Q), BF16),
            dma((8,)), dma((blocks, 4)), dma((blocks, 4)), dma((blocks, 3, 2)), dma((blocks, 3, 2)),
            dma((8,)), dma((8,)), dma((8,)), dma((8,)),
        ],
        compiler_params=pltpu.CompilerParams(
            collective_id=2, has_side_effects=True, vmem_limit_bytes=VMEM_LIMIT
        ),
        name="project",
    )(slots, ylg, eg, cc, inc, gain, down, weight)


def lay_out_kernel(place_ref, panel_ref, out_ref):
    group = out_ref.shape[0]
    for k in range(group):
        place = place_ref[pl.program_id(0) * group + k]
        here = jnp.logical_and(place >= 0, place < PANEL_DEV)
        out_ref[k] = jnp.where(here, panel_ref[jnp.clip(place, 0, PANEL_DEV - 1)], 0)


def lay_out(places, panels, group=8):
    slots = places.shape[0]
    shape = panels.shape[1:]
    return pl.pallas_call(
        lay_out_kernel,
        grid_spec=pltpu.PrefetchScalarGridSpec(
            num_scalar_prefetch=1,
            grid=(slots // group,),
            in_specs=[pl.BlockSpec(panels.shape, lambda i, s: (0, 0, 0))],
            out_specs=pl.BlockSpec((group,) + shape, lambda i, s: (i, 0, 0)),
        ),
        out_shape=jax.ShapeDtypeStruct((slots,) + shape, BF16),
        name="lay_out",
    )(places, panels)


def adapt_kernel(slot_ref, base_ref, low_ref, up_ref, out_ref):
    out_ref[...] = (base_ref[...] + dot_dims(low_ref[0], up_ref[0], 0, 0)).astype(BF16)


def adapt(slots, base, low, up):
    tokens, feat = base.shape
    rank = low.shape[1]
    return pl.pallas_call(
        adapt_kernel,
        grid_spec=pltpu.PrefetchScalarGridSpec(
            num_scalar_prefetch=1,
            grid=(tokens // Q,),
            in_specs=[
                pl.BlockSpec((Q, feat), lambda i, s: (i, 0)),
                pl.BlockSpec((1, rank, Q), lambda i, s: (i, 0, 0)),
                pl.BlockSpec((1, rank, feat), lambda i, s: (s[i], 0, 0)),
            ],
            out_specs=pl.BlockSpec((Q, feat), lambda i, s: (i, 0)),
        ),
        out_shape=jax.ShapeDtypeStruct((tokens, feat), BF16),
        compiler_params=pltpu.CompilerParams(vmem_limit_bytes=16 * 1024 * 1024),
        name="adapt",
    )(slots, base, low, up)


def local(
    input_x_channels,
    input_b_channels,
    input_c_channels,
    input_gate_channels,
    raw_step_sizes,
    log_decay_rate,
    head_skip_coeff,
    x_conv_taps,
    b_conv_taps,
    c_conv_taps,
    gated_norm_gain,
    output_weight,
    adapter_down_panels,
    adapter_up_panels,
    turn_first_token,
    tenant_of_turn,
    tenant_panel_index,
):
    tokens = input_x_channels.shape[0]
    own = lax.axis_index("ctx")
    homes = jnp.take(tenant_panel_index, tenant_of_turn)
    starts = lax.dynamic_slice_in_dim(turn_first_token, TURN_DEV * own, TURN_DEV, 0)
    firsts = own * tokens + Q * jnp.arange(tokens // Q)
    slots = jnp.sum((firsts[:, None] >= starts[None, :]).astype(jnp.int32), axis=1)

    places = homes - PANEL_DEV * own
    offered = lay_out(places, adapter_down_panels.transpose(0, 2, 1))
    count = lax.axis_size("ctx")
    onward = [(i, i + 1) for i in range(count - 1)]
    mine = lax.psum_scatter(offered, "ctx", scatter_dimension=0, tiled=True)

    tails = jnp.concatenate(
        [input_x_channels[tokens - 8 :], input_b_channels[tokens - 8 :], input_c_channels[tokens - 8 :]],
        axis=1,
    )
    halo = lax.ppermute(tails, "ctx", onward)
    ylg, eg, cc, state, decay = local_scan(
        input_x_channels, input_b_channels, input_c_channels, input_gate_channels, raw_step_sizes,
        log_decay_rate, head_skip_coeff, halo, x_conv_taps, b_conv_taps, c_conv_taps,
    )
    inc = exchange(state, decay)
    mine, inc = lax.optimization_barrier((mine, inc))
    before = lax.ppermute(mine[TURN_DEV - 1 :], "ctx", onward)
    down = jnp.concatenate([before, mine], axis=0)
    windows = [max(TURN_DEV * i - 1 + k, 0) for i in range(count) for k in range(TURN_DEV + 1)]
    wanted, up_panels, mine = lax.optimization_barrier(
        (jnp.take(places, jnp.array(windows)), adapter_up_panels, mine)
    )
    up = lax.psum_scatter(lay_out(wanted, up_panels), "ctx", scatter_dimension=0, tiled=True)
    base, low = project(slots, ylg, eg, cc, inc, gated_norm_gain.reshape(1, -1), down, output_weight)
    up, base = lax.optimization_barrier((up, base))
    return adapt(slots, base, low, up)


def solution(mesh):
    in_specs = (
        P("ctx", "head"),
        P("ctx", "head"),
        P("ctx", "head"),
        P("ctx", "head"),
        P("head", "ctx"),
        P("head"),
        P("head"),
        P(None, "head"),
        P(None, "head"),
        P(None, "head"),
        P("head"),
        P("head", None),
        P("ctx", "head", None),
        P("ctx", None, "head"),
        P(),
        P(),
        P(),
    )
    out_specs = P("ctx", "head")
    return jax.shard_map(local, mesh=mesh, in_specs=in_specs, out_specs=out_specs, check_vma=False)
```

```python
import functools

import jax
import jax.numpy as jnp
from jax import lax
from jax.experimental import pallas as pl
from jax.experimental.pallas import tpu as pltpu
from jax.sharding import PartitionSpec as P

P_SIZE = 64
N = 128
Q = 128
TURN_DEV = 2
PANEL_DEV = 6
WAVE_LAG = 3
LOG2E = 1.4426950408889634
EPSILON = 1e-05
VMEM_LIMIT = 60 * 1024 * 1024
MESH = pl.DeviceIdType.MESH
F32 = jnp.float32
BF16 = jnp.bfloat16


def silu(v):
    half = 0.5 * v
    return half + half * jnp.tanh(half)


def dot(a, b):
    return jnp.dot(a, b, preferred_element_type=F32)


def dot_dims(a, b, ca, cb):
    return lax.dot_general(a, b, (((ca,), (cb,)), ((), ())), preferred_element_type=F32)


def scan_kernel(
    rate_ref, skip_ref, x_ref, b_ref, c_ref, z_ref, raw_ref, halo_ref, xt_ref, bt_ref, ct_ref,
    ylg_ref, eg_ref, cc_ref, s_ref, d_ref,
    xp, bp, cp, start, skl,
):
    step = pl.program_id(0)
    heads = raw_ref.shape[0]
    width = x_ref.shape[1]
    lane = lax.broadcasted_iota(jnp.int32, (8, 128), 1)

    @pl.when(step == 0)
    def _():
        xp[0:8, :] = halo_ref[:, 0:width].astype(F32)
        bp[0:8, :] = halo_ref[:, width : width + N].astype(F32)
        cp[0:8, :] = halo_ref[:, width + N : width + 2 * N].astype(F32)
        start[...] = jnp.zeros_like(start)
        s_ref[...] = jnp.zeros_like(s_ref)
        for pair in range(heads // 2):
            skl[:, pair * 128 : pair * 128 + 128] = jnp.where(
                lane < P_SIZE, skip_ref[2 * pair], skip_ref[2 * pair + 1]
            )

    @pl.when(step > 0)
    def _():
        xp[0:8, :] = xp[Q : Q + 8, :]
        bp[0:8, :] = bp[Q : Q + 8, :]
        cp[0:8, :] = cp[Q : Q + 8, :]

    xp[8 : 8 + Q, :] = x_ref[...].astype(F32)
    bp[8 : 8 + Q, :] = b_ref[...].astype(F32)
    cp[8 : 8 + Q, :] = c_ref[...].astype(F32)

    def conv(padded, taps, sl):
        total = taps[0:1, sl].astype(F32) * padded[5 : 5 + Q, sl]
        for k in range(1, 4):
            total = total + taps[k : k + 1, sl].astype(F32) * padded[5 + k : 5 + k + Q, sl]
        return silu(total).astype(BF16)

    every = slice(0, N)
    bc = conv(bp, bt_ref, every)
    cc = conv(cp, ct_ref, every)
    cc_ref[...] = cc
    bt = bc.astype(F32).T.astype(BF16)
    row = lax.broadcasted_iota(jnp.int32, (Q, Q), 0)
    col = lax.broadcasted_iota(jnp.int32, (Q, Q), 1)
    scores = jnp.where(row >= col, dot(cc, bt), 0.0)

    raw = raw_ref[...]
    dt = jnp.maximum(raw, 0.0) + jnp.log1p(jnp.exp(-jnp.abs(raw)))
    hrow = lax.broadcasted_iota(jnp.int32, (heads, Q), 0)
    lrow = lax.broadcasted_iota(jnp.int32, (heads, Q), 1)
    rate = jnp.zeros((heads, Q), F32)
    for h in range(heads):
        rate = jnp.where(hrow == h, rate_ref[h], rate)
    run = -dt * jnp.exp(rate)
    shift = 1
    while shift < Q:
        run = run + jnp.where(lrow >= shift, pltpu.roll(run, shift, 1), 0.0)
        shift *= 2
    run2 = run * LOG2E
    last2 = jnp.broadcast_to(run2[:, Q - 1 : Q], (heads, Q))
    stacked = jnp.concatenate(
        [dt, run2] + [jnp.zeros((heads, Q), F32)] * ((Q - 2 * heads) // heads), axis=0
    )
    tr = stacked.T
    before2 = start[...]
    start[...] = before2 + last2
    half_lane = lax.broadcasted_iota(jnp.int32, (Q, 128), 1) < P_SIZE
    half_row = lax.broadcasted_iota(jnp.int32, (1, 128), 1) < P_SIZE

    for pair in range(heads // 2):
        h0, h1 = 2 * pair, 2 * pair + 1
        sl = slice(pair * 128, pair * 128 + 128)
        xc = conv(xp, xt_ref, sl).astype(F32)
        dt_e = jnp.where(half_lane, tr[:, h0 : h0 + 1], tr[:, h1 : h1 + 1])
        c0 = jnp.broadcast_to(tr[:, heads + h0 : heads + h0 + 1], (Q, Q))
        c1 = jnp.broadcast_to(tr[:, heads + h1 : heads + h1 + 1], (Q, Q))
        run_e = jnp.where(half_lane, c0, c1)
        last_e = jnp.where(half_row, last2[h0 : h0 + 1, :], last2[h1 : h1 + 1, :])
        start_e = jnp.where(half_row, before2[h0 : h0 + 1, :], before2[h1 : h1 + 1, :])
        xdt = xc * dt_e
        m0 = (scores * jnp.exp2(jnp.minimum(c0 - run2[h0 : h0 + 1, :], 0.0))).astype(BF16)
        m1 = (scores * jnp.exp2(jnp.minimum(c1 - run2[h1 : h1 + 1, :], 0.0))).astype(BF16)
        mixing = jnp.concatenate([m0, m1], axis=1)
        xdt_pair = jnp.concatenate(
            [jnp.where(half_lane, xdt, 0.0), jnp.where(half_lane, 0.0, xdt)], axis=0
        ).astype(BF16)
        grow = jnp.exp2(run_e)
        carried = s_ref[:, sl]
        y = dot(mixing, xdt_pair) + grow * dot(cc, carried.astype(BF16)) + skl[0:1, sl] * xc
        gate = silu(z_ref[:, sl].astype(F32))
        ylg_ref[:, sl] = (y * gate).astype(BF16)
        eg_ref[:, sl] = (grow * jnp.exp2(start_e) * gate).astype(BF16)
        weighted = (xdt * jnp.exp2(last_e - run_e)).astype(BF16)
        s_ref[:, sl] = jnp.exp2(last_e) * carried + dot(bt, weighted)
        d_ref[:, sl] = jnp.broadcast_to(jnp.exp2(start_e + last_e), (8, 128))


def local_scan(x, b, c, z, raw, rate, skip, halo, xt, bt, ct):
    tokens, width = x.shape
    heads = raw.shape[0]
    smem = pl.BlockSpec(memory_space=pltpu.SMEM)
    whole = lambda a: pl.BlockSpec(a.shape, lambda i: (0,) * a.ndim)
    rows = lambda w: pl.BlockSpec((Q, w), lambda i: (i, 0))
    return pl.pallas_call(
        scan_kernel,
        grid=(tokens // Q,),
        in_specs=[
            smem, smem, rows(width), rows(N), rows(N), rows(width),
            pl.BlockSpec((heads, Q), lambda i: (0, i)),
            whole(halo), whole(xt), whole(bt), whole(ct),
        ],
        out_specs=[
            rows(width), rows(width), rows(N),
            pl.BlockSpec((N, width), lambda i: (0, 0)),
            pl.BlockSpec((8, width), lambda i: (0, 0)),
        ],
        out_shape=[
            jax.ShapeDtypeStruct((tokens, width), BF16),
            jax.ShapeDtypeStruct((tokens, width), BF16),
            jax.ShapeDtypeStruct((tokens, N), BF16),
            jax.ShapeDtypeStruct((N, width), F32),
            jax.ShapeDtypeStruct((8, width), F32),
        ],
        scratch_shapes=[
            pltpu.VMEM((Q + 8, width), F32),
            pltpu.VMEM((Q + 8, N), F32),
            pltpu.VMEM((Q + 8, N), F32),
            pltpu.VMEM((heads, Q), F32),
            pltpu.VMEM((8, width), F32),
        ],
        compiler_params=pltpu.CompilerParams(
            dimension_semantics=("arbitrary",), vmem_limit_bytes=VMEM_LIMIT
        ),
        name="local_scan",
    )(rate, skip, x, b, c, z, raw, halo, xt, bt, ct)


def partners():
    me = lax.axis_index("ctx")
    x, z = me // 4, me % 4
    return [
        (x * 4 + (z + 1 - 2 * (z % 2)), z % 2),
        (x * 4 + (3 - z), z // 2),
        ((x + 1 - 2 * (x % 2)) * 4 + z, x % 2),
        ((3 - x) * 4 + z, x // 2),
    ]


def exchange_kernel(
    s_ref, d_ref, inc_ref, total, prefix, decay, dsend, drecv, ssend, srecv,
    sem_ds, sem_dr, sem_ss, sem_sr, *, chunks,
):
    steps = partners()
    barrier = pltpu.get_barrier_semaphore()
    for other, _ in steps:
        pl.semaphore_signal(barrier, inc=1, device_id={"ctx": other}, device_id_type=MESH)
    width = s_ref.shape[1]
    cw = width // chunks

    def state_copy(c, s):
        return pltpu.make_async_remote_copy(
            src_ref=ssend.at[s, c], dst_ref=srecv.at[s, c],
            send_sem=sem_ss.at[s, c], recv_sem=sem_sr.at[s, c],
            device_id={"ctx": steps[s][0]}, device_id_type=MESH,
        )

    def decay_copy(s):
        return pltpu.make_async_remote_copy(
            src_ref=dsend.at[s], dst_ref=drecv.at[s],
            send_sem=sem_ds.at[s], recv_sem=sem_dr.at[s],
            device_id={"ctx": steps[s][0]}, device_id_type=MESH,
        )

    for c in range(chunks):
        ssend[0, c] = s_ref[:, c * cw : c * cw + cw].astype(BF16)
    dsend[0] = d_ref[...]
    total[...] = s_ref[...]
    prefix[...] = jnp.zeros_like(prefix)
    pl.semaphore_wait(barrier, len(steps))
    decay_copy(0).start()
    for c in range(chunks):
        state_copy(c, 0).start()
    decay[0] = d_ref[...]
    decay[1] = jnp.ones_like(d_ref)
    for wave in range(chunks + 3 * WAVE_LAG):
        for s in range(4):
            c = wave - WAVE_LAG * s
            if c < 0 or c >= chunks:
                continue
            sl = slice(c * cw, c * cw + cw)
            upper = steps[s][1] == 1
            if c == 0:
                decay_copy(s).wait_recv()
                theirs = drecv[s]
                decay[2 * s + 2] = decay[2 * s] * theirs
                decay[2 * s + 3] = decay[2 * s + 1] * jnp.where(upper, theirs, 1.0)
                if s < 3:
                    dsend[s + 1] = decay[2 * s + 2]
                    decay_copy(s + 1).start()
            state_copy(c, s).wait_recv()
            incoming = srecv[s, c].astype(F32)
            mine = decay[2 * s, 0:1, sl]
            ahead = decay[2 * s + 1, 0:1, sl]
            theirs = drecv[s, 0:1, sl]
            prefix[:, sl] = prefix[:, sl] + jnp.where(upper, ahead, 0.0) * incoming
            if s < 3:
                new = (
                    jnp.where(upper, mine, 1.0) * incoming
                    + jnp.where(upper, 1.0, theirs) * total[:, sl]
                )
                total[:, sl] = new
                ssend[s + 1, c] = new.astype(BF16)
                state_copy(c, s + 1).start()
    inc_ref[...] = prefix[...].astype(BF16)
    for s in range(4):
        decay_copy(s).wait_send()
        for c in range(chunks):
            state_copy(c, s).wait_send()


def exchange(state, decay, chunks=8):
    width = state.shape[1]
    cw = width // chunks
    vmem = pl.BlockSpec(memory_space=pltpu.VMEM)
    return pl.pallas_call(
        functools.partial(exchange_kernel, chunks=chunks),
        in_specs=[vmem, vmem],
        out_specs=vmem,
        out_shape=jax.ShapeDtypeStruct((N, width), BF16),
        scratch_shapes=[
            pltpu.VMEM((N, width), F32),
            pltpu.VMEM((N, width), F32),
            pltpu.VMEM((10, 8, width), F32),
            pltpu.VMEM((4, 8, width), F32),
            pltpu.VMEM((4, 8, width), F32),
            pltpu.VMEM((4, chunks, N, cw), BF16),
            pltpu.VMEM((4, chunks, N, cw), BF16),
            pltpu.SemaphoreType.DMA((4,)),
            pltpu.SemaphoreType.DMA((4,)),
            pltpu.SemaphoreType.DMA((4, chunks)),
            pltpu.SemaphoreType.DMA((4, chunks)),
        ],
        compiler_params=pltpu.CompilerParams(
            collective_id=1, has_side_effects=True, vmem_limit_bytes=VMEM_LIMIT
        ),
        name="state_exchange",
    )(state, decay)


LAG = (1, 2, 3, 4)


def project_kernel(
    ylg_ref, eg_ref, cc_ref, inc_ref, gain_ref, w_ref,
    base_ref, normed_ref,
    wv, own, psend, precv, rsend, rrecv,
    sem_w, sem_ps, sem_pr, sem_rs, sem_rr,
):
    head = lax.axis_index("head")
    y, core = head // 2, head % 2
    blocks = ylg_ref.shape[0] // Q
    feat = base_ref.shape[1]
    half = Q // 2
    barrier = pltpu.get_barrier_semaphore()
    for k in range(1, 8):
        pl.semaphore_signal(
            barrier, inc=1, device_id={"head": (head + k) % 8}, device_id_type=MESH
        )

    dests = [(y + 3) % 4, (y + 1) % 4, (y + 2) % 4, y]

    def w_copy(d, side):
        index = d * 2 + side
        at = pl.multiple_of(index * feat, feat)
        return pltpu.make_async_copy(w_ref.at[:, pl.ds(at, feat)], wv.at[index], sem_w.at[index])

    for d in dests:
        for side in (1 - core, core):
            w_copy(d, side).start()

    def pair_copy(b, d):
        return pltpu.make_async_remote_copy(
            src_ref=psend.at[b, d], dst_ref=precv.at[b, d],
            send_sem=sem_ps.at[b, d], recv_sem=sem_pr.at[b, d],
            device_id={"head": y * 2 + 1 - core}, device_id_type=MESH,
        )

    def ring_copy(b, j, way):
        to = (y + 1 + 2 * way) % 4
        return pltpu.make_async_remote_copy(
            src_ref=rsend.at[b, j, way], dst_ref=rrecv.at[b, j, way],
            send_sem=sem_rs.at[b, j, way], recv_sem=sem_rr.at[b, j, way],
            device_id={"head": to * 2 + core}, device_id_type=MESH,
        )

    pl.semaphore_wait(barrier, 7)

    def compute(b):
        rows = pl.ds(pl.multiple_of(b * Q, Q), Q)
        got = dot(cc_ref[rows, :], inc_ref[...])
        gated = ylg_ref[rows, :].astype(F32) + eg_ref[rows, :].astype(F32) * got
        scale = lax.rsqrt(jnp.mean(gated * gated, axis=1, keepdims=True) + EPSILON)
        normed = (gated * scale * gain_ref[...].astype(F32)).astype(BF16)
        normed_ref[rows, :] = normed
        for d in dests:
            @pl.when(b == 0)
            def _():
                w_copy(d, 1 - core).wait()
            psend[b, d] = dot(normed, wv[d * 2 + 1 - core]).astype(BF16)
            pair_copy(b, d).start()

            @pl.when(b == 0)
            def _():
                w_copy(d, core).wait()
            own[b, d] = dot(normed, wv[d * 2 + core])

    def ring(b, j):
        if j == 0:
            pair_copy(b, dests[0]).wait_recv()
            pair_copy(b, dests[1]).wait_recv()
        elif j == 1:
            pair_copy(b, dests[2]).wait_recv()
        elif j == 3:
            pair_copy(b, dests[3]).wait_recv()
        for way in range(2):
            d = (y + (j + 1) * (3 - 2 * way)) % 4
            part = slice(way * half, way * half + half)
            value = own[b, d, part, :] + precv[b, d, part, :].astype(F32)
            if j > 0:
                ring_copy(b, j - 1, way).wait_recv()
                value = value + rrecv[b, j - 1, way].astype(F32)
            if j < 3:
                rsend[b, j, way] = value.astype(BF16)
                ring_copy(b, j, way).start()
            else:
                at = pl.multiple_of(b * Q + way * half, half)
                base_ref[pl.ds(at, half), :] = value

    def tick(t, carry):
        @pl.when(t < blocks)
        def _():
            compute(t)

        for j in range(4):
            b = t - LAG[j]

            @pl.when(jnp.logical_and(b >= 0, b < blocks))
            def _():
                ring(b, j)

        return carry

    lax.fori_loop(0, blocks + LAG[3], tick, 0)

    def drain(b, carry):
        for d in range(4):
            pair_copy(b, d).wait_send()
        for j in range(3):
            for way in range(2):
                ring_copy(b, j, way).wait_send()
        return carry

    lax.fori_loop(0, blocks, drain, 0)


def project(ylg, eg, cc, inc, gain, weight):
    tokens, width = ylg.shape
    feat = weight.shape[1] // 8
    blocks = tokens // Q
    vmem = pl.BlockSpec(memory_space=pltpu.VMEM)
    dma = pltpu.SemaphoreType.DMA
    return pl.pallas_call(
        project_kernel,
        in_specs=[vmem] * 5 + [pl.BlockSpec(memory_space=pl.ANY)],
        out_specs=[vmem, vmem],
        out_shape=[
            jax.ShapeDtypeStruct((tokens, feat), F32),
            jax.ShapeDtypeStruct((tokens, width), BF16),
        ],
        scratch_shapes=[
            pltpu.VMEM((8, width, feat), BF16),
            pltpu.VMEM((blocks, 4, Q, feat), F32),
            pltpu.VMEM((blocks, 4, Q, feat), BF16),
            pltpu.VMEM((blocks, 4, Q, feat), BF16),
            pltpu.VMEM((blocks, 3, 2, Q // 2, feat), BF16),
            pltpu.VMEM((blocks, 3, 2, Q // 2, feat), BF16),
            dma((8,)), dma((blocks, 4)), dma((blocks, 4)), dma((blocks, 3, 2)), dma((blocks, 3, 2)),
        ],
        compiler_params=pltpu.CompilerParams(
            collective_id=2, has_side_effects=True, vmem_limit_bytes=VMEM_LIMIT
        ),
        name="project",
    )(ylg, eg, cc, inc, gain, weight)


def lowrank_kernel(
    slot_ref, normed_ref, panel_ref, low_ref, lsend, lrecv, lout, sem_ls, sem_lr, sem_as, sem_ar
):
    head = lax.axis_index("head")
    width = normed_ref.shape[1]
    barrier = pltpu.get_barrier_semaphore()
    for k in range(1, 8):
        pl.semaphore_signal(
            barrier, inc=1, device_id={"head": (head + k) % 8}, device_id_type=MESH
        )

    def low_copy(b):
        return pltpu.make_async_remote_copy(
            src_ref=lsend.at[b], dst_ref=lrecv.at[head],
            send_sem=sem_ls.at[b], recv_sem=sem_lr.at[head],
            device_id={"head": b}, device_id_type=MESH,
        )

    def low_arrival(k):
        return pltpu.make_async_remote_copy(
            src_ref=lsend.at[k], dst_ref=lrecv.at[k],
            send_sem=sem_ls.at[k], recv_sem=sem_lr.at[k],
            device_id={"head": k}, device_id_type=MESH,
        )

    def sum_copy(k):
        return pltpu.make_async_remote_copy(
            src_ref=lout.at[head], dst_ref=lout.at[head],
            send_sem=sem_as.at[k], recv_sem=sem_ar.at[head],
            device_id={"head": k}, device_id_type=MESH,
        )

    def sum_arrival(k):
        return pltpu.make_async_remote_copy(
            src_ref=lout.at[k], dst_ref=lout.at[k],
            send_sem=sem_as.at[k], recv_sem=sem_ar.at[k],
            device_id={"head": k}, device_id_type=MESH,
        )

    pl.semaphore_wait(barrier, 7)
    for b in range(8):
        low = dot_dims(
            panel_ref[slot_ref[b], :, 0:width], normed_ref[b * Q : b * Q + Q, :], 1, 1
        ).astype(BF16)
        lsend[b] = low

        @pl.when(b == head)
        def _():
            lrecv[b] = low

        @pl.when(b != head)
        def _():
            low_copy(b).start()

    for k in range(8):
        @pl.when(k != head)
        def _():
            low_arrival(k).wait_recv()
    total = lrecv[0].astype(F32)
    for k in range(1, 8):
        total = total + lrecv[k].astype(F32)
    lout[head] = total.astype(BF16)
    for k in range(8):
        @pl.when(k != head)
        def _():
            sum_copy(k).start()

    for k in range(8):
        @pl.when(k != head)
        def _():
            sum_arrival(k).wait_recv()
            low_copy(k).wait_send()
            sum_copy(k).wait_send()
    low_ref[...] = lout[...]


def lowrank(slots, normed, panels):
    rank = panels.shape[1]
    vmem = pl.BlockSpec(memory_space=pltpu.VMEM)
    dma = pltpu.SemaphoreType.DMA
    return pl.pallas_call(
        lowrank_kernel,
        in_specs=[pl.BlockSpec(memory_space=pltpu.SMEM), vmem, vmem],
        out_specs=vmem,
        out_shape=jax.ShapeDtypeStruct((8, rank, Q), BF16),
        scratch_shapes=[pltpu.VMEM((8, rank, Q), BF16)] * 3 + [dma((8,))] * 4,
        compiler_params=pltpu.CompilerParams(
            collective_id=3, has_side_effects=True, vmem_limit_bytes=16 * 1024 * 1024
        ),
        name="lowrank",
    )(slots, normed, panels)


SLOTS = TURN_DEV + 1


def lay_out_kernel(tenant_ref, index_ref, down_ref, up_ref, out_ref):
    group, width = out_ref.shape[0], down_ref.shape[2]
    first = PANEL_DEV * lax.axis_index("ctx")
    for k in range(group):
        device = pl.program_id(0) * (group // SLOTS) + k // SLOTS
        turn = jnp.maximum(TURN_DEV * device - 1 + k % SLOTS, 0)
        place = index_ref[tenant_ref[turn]] - first
        here = jnp.logical_and(place >= 0, place < PANEL_DEV)
        at = jnp.clip(place, 0, PANEL_DEV - 1)
        out_ref[k, :, 0:width] = jnp.where(here, down_ref[at], 0)
        out_ref[k, :, width:] = jnp.where(here, up_ref[at], 0)


def lay_out(tenants, index, down, up, devices, group=2 * SLOTS):
    rank, width = down.shape[1:]
    total = width + up.shape[2]
    return pl.pallas_call(
        lay_out_kernel,
        grid_spec=pltpu.PrefetchScalarGridSpec(
            num_scalar_prefetch=2,
            grid=(devices * SLOTS // group,),
            in_specs=[
                pl.BlockSpec(down.shape, lambda i, *s: (0, 0, 0)),
                pl.BlockSpec(up.shape, lambda i, *s: (0, 0, 0)),
            ],
            out_specs=pl.BlockSpec((group, rank, total), lambda i, *s: (i, 0, 0)),
        ),
        out_shape=jax.ShapeDtypeStruct((devices * SLOTS, rank, total), BF16),
        name="lay_out",
    )(tenants, index, down, up)


def adapt_kernel(slot_ref, base_ref, low_ref, up_ref, out_ref):
    out_ref[...] = (base_ref[...] + dot_dims(low_ref[0], up_ref[0], 0, 0)).astype(BF16)


def adapt(slots, base, low, up):
    tokens, feat = base.shape
    rank = low.shape[1]
    return pl.pallas_call(
        adapt_kernel,
        grid_spec=pltpu.PrefetchScalarGridSpec(
            num_scalar_prefetch=1,
            grid=(tokens // Q,),
            in_specs=[
                pl.BlockSpec((Q, feat), lambda i, s: (i, 0)),
                pl.BlockSpec((1, rank, Q), lambda i, s: (i, 0, 0)),
                pl.BlockSpec((1, rank, feat), lambda i, s: (s[i], 0, up.shape[2] // feat - 1)),
            ],
            out_specs=pl.BlockSpec((Q, feat), lambda i, s: (i, 0)),
        ),
        out_shape=jax.ShapeDtypeStruct((tokens, feat), BF16),
        compiler_params=pltpu.CompilerParams(vmem_limit_bytes=16 * 1024 * 1024),
        name="adapt",
    )(slots, base, low, up)


def local(
    input_x_channels,
    input_b_channels,
    input_c_channels,
    input_gate_channels,
    raw_step_sizes,
    log_decay_rate,
    head_skip_coeff,
    x_conv_taps,
    b_conv_taps,
    c_conv_taps,
    gated_norm_gain,
    output_weight,
    adapter_down_panels,
    adapter_up_panels,
    turn_first_token,
    tenant_of_turn,
    tenant_panel_index,
):
    tokens = input_x_channels.shape[0]
    own = lax.axis_index("ctx")
    starts = lax.dynamic_slice_in_dim(turn_first_token, TURN_DEV * own, TURN_DEV, 0)
    firsts = own * tokens + Q * jnp.arange(tokens // Q)
    slots = jnp.sum((firsts[:, None] >= starts[None, :]).astype(jnp.int32), axis=1)

    count = lax.axis_size("ctx")
    offered = lay_out(
        tenant_of_turn, tenant_panel_index,
        adapter_down_panels.transpose(0, 2, 1), adapter_up_panels, count,
    )
    panels = lax.psum_scatter(offered, "ctx", scatter_dimension=0, tiled=True)

    tails = jnp.concatenate(
        [input_x_channels[tokens - 8 :], input_b_channels[tokens - 8 :], input_c_channels[tokens - 8 :]],
        axis=1,
    )
    halo = lax.ppermute(tails, "ctx", [(i, i + 1) for i in range(count - 1)])
    ylg, eg, cc, state, decay = local_scan(
        input_x_channels, input_b_channels, input_c_channels, input_gate_channels, raw_step_sizes,
        log_decay_rate, head_skip_coeff, halo, x_conv_taps, b_conv_taps, c_conv_taps,
    )
    inc = exchange(state, decay)
    base, normed = project(ylg, eg, cc, inc, gated_norm_gain.reshape(1, -1), output_weight)
    panels, normed = lax.optimization_barrier((panels, normed))
    low = lowrank(slots, normed, panels)
    return adapt(slots, base, low, panels)


def solution(mesh):
    in_specs = (
        P("ctx", "head"),
        P("ctx", "head"),
        P("ctx", "head"),
        P("ctx", "head"),
        P("head", "ctx"),
        P("head"),
        P("head"),
        P(None, "head"),
        P(None, "head"),
        P(None, "head"),
        P("head"),
        P("head", None),
        P("ctx", "head", None),
        P("ctx", None, "head"),
        P(),
        P(),
        P(),
    )
    out_specs = P("ctx", "head")
    return jax.shard_map(local, mesh=mesh, in_specs=in_specs, out_specs=out_specs, check_vma=False)
```

```python
import functools

import jax
import jax.numpy as jnp
from jax import lax
from jax.experimental import pallas as pl
from jax.experimental.pallas import tpu as pltpu
from jax.sharding import PartitionSpec as P

P_SIZE = 64
N = 128
Q = 128
TURN_DEV = 2
PANEL_DEV = 6
WAVE_LAG = 3
LOG2E = 1.4426950408889634
EPSILON = 1e-05
VMEM_LIMIT = 60 * 1024 * 1024
MESH = pl.DeviceIdType.MESH
F32 = jnp.float32
BF16 = jnp.bfloat16


def silu(v):
    half = 0.5 * v
    return half + half * jnp.tanh(half)


def dot(a, b):
    return jnp.dot(a, b, preferred_element_type=F32)


def dot_dims(a, b, ca, cb):
    return lax.dot_general(a, b, (((ca,), (cb,)), ((), ())), preferred_element_type=F32)


def scan_kernel(
    rate_ref, skip_ref, x_ref, b_ref, c_ref, z_ref, raw_ref, halo_ref, xt_ref, bt_ref, ct_ref,
    ylg_ref, eg_ref, cc_ref, s_ref, d_ref,
    xp, bp, cp, start, skl,
):
    step = pl.program_id(0)
    heads = raw_ref.shape[0]
    width = x_ref.shape[1]
    lane = lax.broadcasted_iota(jnp.int32, (8, 128), 1)

    @pl.when(step == 0)
    def _():
        xp[0:8, :] = halo_ref[:, 0:width].astype(F32)
        bp[0:8, :] = halo_ref[:, width : width + N].astype(F32)
        cp[0:8, :] = halo_ref[:, width + N : width + 2 * N].astype(F32)
        start[...] = jnp.zeros_like(start)
        s_ref[...] = jnp.zeros_like(s_ref)
        for pair in range(heads // 2):
            skl[:, pair * 128 : pair * 128 + 128] = jnp.where(
                lane < P_SIZE, skip_ref[2 * pair], skip_ref[2 * pair + 1]
            )

    @pl.when(step > 0)
    def _():
        xp[0:8, :] = xp[Q : Q + 8, :]
        bp[0:8, :] = bp[Q : Q + 8, :]
        cp[0:8, :] = cp[Q : Q + 8, :]

    xp[8 : 8 + Q, :] = x_ref[...].astype(F32)
    bp[8 : 8 + Q, :] = b_ref[...].astype(F32)
    cp[8 : 8 + Q, :] = c_ref[...].astype(F32)

    def conv(padded, taps, sl):
        total = taps[0:1, sl].astype(F32) * padded[5 : 5 + Q, sl]
        for k in range(1, 4):
            total = total + taps[k : k + 1, sl].astype(F32) * padded[5 + k : 5 + k + Q, sl]
        return silu(total).astype(BF16)

    every = slice(0, N)
    bc = conv(bp, bt_ref, every)
    cc = conv(cp, ct_ref, every)
    cc_ref[...] = cc
    bt = bc.astype(F32).T.astype(BF16)
    row = lax.broadcasted_iota(jnp.int32, (Q, Q), 0)
    col = lax.broadcasted_iota(jnp.int32, (Q, Q), 1)
    scores = jnp.where(row >= col, dot(cc, bt), 0.0)

    raw = raw_ref[...]
    dt = jnp.maximum(raw, 0.0) + jnp.log1p(jnp.exp(-jnp.abs(raw)))
    hrow = lax.broadcasted_iota(jnp.int32, (heads, Q), 0)
    lrow = lax.broadcasted_iota(jnp.int32, (heads, Q), 1)
    rate = jnp.zeros((heads, Q), F32)
    for h in range(heads):
        rate = jnp.where(hrow == h, rate_ref[h], rate)
    run = -dt * jnp.exp(rate)
    shift = 1
    while shift < Q:
        run = run + jnp.where(lrow >= shift, pltpu.roll(run, shift, 1), 0.0)
        shift *= 2
    run2 = run * LOG2E
    last2 = jnp.broadcast_to(run2[:, Q - 1 : Q], (heads, Q))
    stacked = jnp.concatenate(
        [dt, run2] + [jnp.zeros((heads, Q), F32)] * ((Q - 2 * heads) // heads), axis=0
    )
    tr = stacked.T
    before2 = start[...]
    start[...] = before2 + last2
    half_lane = lax.broadcasted_iota(jnp.int32, (Q, 128), 1) < P_SIZE
    half_row = lax.broadcasted_iota(jnp.int32, (1, 128), 1) < P_SIZE

    for pair in range(heads // 2):
        h0, h1 = 2 * pair, 2 * pair + 1
        sl = slice(pair * 128, pair * 128 + 128)
        xc = conv(xp, xt_ref, sl).astype(F32)
        dt_e = jnp.where(half_lane, tr[:, h0 : h0 + 1], tr[:, h1 : h1 + 1])
        c0 = jnp.broadcast_to(tr[:, heads + h0 : heads + h0 + 1], (Q, Q))
        c1 = jnp.broadcast_to(tr[:, heads + h1 : heads + h1 + 1], (Q, Q))
        run_e = jnp.where(half_lane, c0, c1)
        last_e = jnp.where(half_row, last2[h0 : h0 + 1, :], last2[h1 : h1 + 1, :])
        start_e = jnp.where(half_row, before2[h0 : h0 + 1, :], before2[h1 : h1 + 1, :])
        xdt = xc * dt_e
        m0 = (scores * jnp.exp2(jnp.minimum(c0 - run2[h0 : h0 + 1, :], 0.0))).astype(BF16)
        m1 = (scores * jnp.exp2(jnp.minimum(c1 - run2[h1 : h1 + 1, :], 0.0))).astype(BF16)
        mixing = jnp.concatenate([m0, m1], axis=1)
        xdt_pair = jnp.concatenate(
            [jnp.where(half_lane, xdt, 0.0), jnp.where(half_lane, 0.0, xdt)], axis=0
        ).astype(BF16)
        grow = jnp.exp2(run_e)
        carried = s_ref[:, sl]
        y = dot(mixing, xdt_pair) + grow * dot(cc, carried.astype(BF16)) + skl[0:1, sl] * xc
        gate = silu(z_ref[:, sl].astype(F32))
        ylg_ref[:, sl] = (y * gate).astype(BF16)
        eg_ref[:, sl] = (grow * jnp.exp2(start_e) * gate).astype(BF16)
        weighted = (xdt * jnp.exp2(last_e - run_e)).astype(BF16)
        s_ref[:, sl] = jnp.exp2(last_e) * carried + dot(bt, weighted)
        d_ref[:, sl] = jnp.broadcast_to(jnp.exp2(start_e + last_e), (8, 128))


def local_scan(x, b, c, z, raw, rate, skip, halo, xt, bt, ct):
    tokens, width = x.shape
    heads = raw.shape[0]
    smem = pl.BlockSpec(memory_space=pltpu.SMEM)
    whole = lambda a: pl.BlockSpec(a.shape, lambda i: (0,) * a.ndim)
    rows = lambda w: pl.BlockSpec((Q, w), lambda i: (i, 0))
    return pl.pallas_call(
        scan_kernel,
        grid=(tokens // Q,),
        in_specs=[
            smem, smem, rows(width), rows(N), rows(N), rows(width),
            pl.BlockSpec((heads, Q), lambda i: (0, i)),
            whole(halo), whole(xt), whole(bt), whole(ct),
        ],
        out_specs=[
            rows(width), rows(width), rows(N),
            pl.BlockSpec((N, width), lambda i: (0, 0)),
            pl.BlockSpec((8, width), lambda i: (0, 0)),
        ],
        out_shape=[
            jax.ShapeDtypeStruct((tokens, width), BF16),
            jax.ShapeDtypeStruct((tokens, width), BF16),
            jax.ShapeDtypeStruct((tokens, N), BF16),
            jax.ShapeDtypeStruct((N, width), F32),
            jax.ShapeDtypeStruct((8, width), F32),
        ],
        scratch_shapes=[
            pltpu.VMEM((Q + 8, width), F32),
            pltpu.VMEM((Q + 8, N), F32),
            pltpu.VMEM((Q + 8, N), F32),
            pltpu.VMEM((heads, Q), F32),
            pltpu.VMEM((8, width), F32),
        ],
        compiler_params=pltpu.CompilerParams(
            dimension_semantics=("arbitrary",), vmem_limit_bytes=VMEM_LIMIT
        ),
        name="local_scan",
    )(rate, skip, x, b, c, z, raw, halo, xt, bt, ct)


def partners():
    me = lax.axis_index("ctx")
    x, z = me // 4, me % 4
    return [
        (x * 4 + (z + 1 - 2 * (z % 2)), z % 2),
        (x * 4 + (3 - z), z // 2),
        ((x + 1 - 2 * (x % 2)) * 4 + z, x % 2),
        ((3 - x) * 4 + z, x // 2),
    ]


def exchange_kernel(
    s_ref, d_ref, inc_ref, total, prefix, decay, dsend, drecv, ssend, srecv,
    sem_ds, sem_dr, sem_ss, sem_sr, *, chunks,
):
    steps = partners()
    barrier = pltpu.get_barrier_semaphore()
    for other, _ in steps:
        pl.semaphore_signal(barrier, inc=1, device_id={"ctx": other}, device_id_type=MESH)
    width = s_ref.shape[1]
    cw = width // chunks

    def state_copy(c, s):
        return pltpu.make_async_remote_copy(
            src_ref=ssend.at[s, c], dst_ref=srecv.at[s, c],
            send_sem=sem_ss.at[s, c], recv_sem=sem_sr.at[s, c],
            device_id={"ctx": steps[s][0]}, device_id_type=MESH,
        )

    def decay_copy(s):
        return pltpu.make_async_remote_copy(
            src_ref=dsend.at[s], dst_ref=drecv.at[s],
            send_sem=sem_ds.at[s], recv_sem=sem_dr.at[s],
            device_id={"ctx": steps[s][0]}, device_id_type=MESH,
        )

    for c in range(chunks):
        ssend[0, c] = s_ref[:, c * cw : c * cw + cw].astype(BF16)
    dsend[0] = d_ref[...]
    total[...] = s_ref[...]
    prefix[...] = jnp.zeros_like(prefix)
    pl.semaphore_wait(barrier, len(steps))
    decay_copy(0).start()
    for c in range(chunks):
        state_copy(c, 0).start()
    decay[0] = d_ref[...]
    decay[1] = jnp.ones_like(d_ref)
    for wave in range(chunks + 3 * WAVE_LAG):
        for s in range(4):
            c = wave - WAVE_LAG * s
            if c < 0 or c >= chunks:
                continue
            sl = slice(c * cw, c * cw + cw)
            upper = steps[s][1] == 1
            if c == 0:
                decay_copy(s).wait_recv()
                theirs = drecv[s]
                decay[2 * s + 2] = decay[2 * s] * theirs
                decay[2 * s + 3] = decay[2 * s + 1] * jnp.where(upper, theirs, 1.0)
                if s < 3:
                    dsend[s + 1] = decay[2 * s + 2]
                    decay_copy(s + 1).start()
            state_copy(c, s).wait_recv()
            incoming = srecv[s, c].astype(F32)
            mine = decay[2 * s, 0:1, sl]
            ahead = decay[2 * s + 1, 0:1, sl]
            theirs = drecv[s, 0:1, sl]
            prefix[:, sl] = prefix[:, sl] + jnp.where(upper, ahead, 0.0) * incoming
            if s < 3:
                new = (
                    jnp.where(upper, mine, 1.0) * incoming
                    + jnp.where(upper, 1.0, theirs) * total[:, sl]
                )
                total[:, sl] = new
                ssend[s + 1, c] = new.astype(BF16)
                state_copy(c, s + 1).start()
    inc_ref[...] = prefix[...].astype(BF16)
    for s in range(4):
        decay_copy(s).wait_send()
        for c in range(chunks):
            state_copy(c, s).wait_send()


def exchange(state, decay, chunks=8):
    width = state.shape[1]
    cw = width // chunks
    vmem = pl.BlockSpec(memory_space=pltpu.VMEM)
    return pl.pallas_call(
        functools.partial(exchange_kernel, chunks=chunks),
        in_specs=[vmem, vmem],
        out_specs=vmem,
        out_shape=jax.ShapeDtypeStruct((N, width), BF16),
        scratch_shapes=[
            pltpu.VMEM((N, width), F32),
            pltpu.VMEM((N, width), F32),
            pltpu.VMEM((10, 8, width), F32),
            pltpu.VMEM((4, 8, width), F32),
            pltpu.VMEM((4, 8, width), F32),
            pltpu.VMEM((4, chunks, N, cw), BF16),
            pltpu.VMEM((4, chunks, N, cw), BF16),
            pltpu.SemaphoreType.DMA((4,)),
            pltpu.SemaphoreType.DMA((4,)),
            pltpu.SemaphoreType.DMA((4, chunks)),
            pltpu.SemaphoreType.DMA((4, chunks)),
        ],
        compiler_params=pltpu.CompilerParams(
            collective_id=1, has_side_effects=True, vmem_limit_bytes=VMEM_LIMIT
        ),
        name="state_exchange",
    )(state, decay)


LAG = (1, 2, 3)


def project_kernel(
    ylg_ref, eg_ref, cc_ref, inc_ref, gain_ref, w_ref,
    base_ref, normed_ref,
    wv, own, psend, precv, hsend, hrecv, fsend, frecv,
    sem_w, sem_ps, sem_pr, sem_hs, sem_hr, sem_fs, sem_fr,
):
    head = lax.axis_index("head")
    y, core = head // 2, head % 2
    blocks = ylg_ref.shape[0] // Q
    feat = base_ref.shape[1]
    half = Q // 2
    barrier = pltpu.get_barrier_semaphore()
    for k in range(1, 8):
        pl.semaphore_signal(
            barrier, inc=1, device_id={"head": (head + k) % 8}, device_id_type=MESH
        )

    dests = [(y + 2) % 4, (y + 1) % 4, (y + 3) % 4, y]

    def w_copy(d, side):
        index = d * 2 + side
        at = pl.multiple_of(index * feat, feat)
        return pltpu.make_async_copy(w_ref.at[:, pl.ds(at, feat)], wv.at[index], sem_w.at[index])

    for d in dests:
        for side in (1 - core, core):
            w_copy(d, side).start()

    def pair_copy(b, d):
        return pltpu.make_async_remote_copy(
            src_ref=psend.at[b, d], dst_ref=precv.at[b, d],
            send_sem=sem_ps.at[b, d], recv_sem=sem_pr.at[b, d],
            device_id={"head": y * 2 + 1 - core}, device_id_type=MESH,
        )

    def half_copy(b, way):
        return pltpu.make_async_remote_copy(
            src_ref=hsend.at[b, way], dst_ref=hrecv.at[b, way],
            send_sem=sem_hs.at[b, way], recv_sem=sem_hr.at[b, way],
            device_id={"head": (y + 1 + 2 * way) % 4 * 2 + core}, device_id_type=MESH,
        )

    def full_copy(b, way):
        return pltpu.make_async_remote_copy(
            src_ref=fsend.at[b, way], dst_ref=frecv.at[b, way],
            send_sem=sem_fs.at[b, way], recv_sem=sem_fr.at[b, way],
            device_id={"head": (y + 1 + 2 * way) % 4 * 2 + core}, device_id_type=MESH,
        )

    pl.semaphore_wait(barrier, 7)

    def compute(b):
        rows = pl.ds(pl.multiple_of(b * Q, Q), Q)
        got = dot(cc_ref[rows, :], inc_ref[...])
        gated = ylg_ref[rows, :].astype(F32) + eg_ref[rows, :].astype(F32) * got
        scale = lax.rsqrt(jnp.mean(gated * gated, axis=1, keepdims=True) + EPSILON)
        normed = (gated * scale * gain_ref[...].astype(F32)).astype(BF16)
        normed_ref[rows, :] = normed
        for d in dests:
            @pl.when(b == 0)
            def _():
                w_copy(d, 1 - core).wait()
            psend[b, d] = dot(normed, wv[d * 2 + 1 - core]).astype(BF16)
            pair_copy(b, d).start()

            @pl.when(b == 0)
            def _():
                w_copy(d, core).wait()
            own[b, d] = dot(normed, wv[d * 2 + core])

    def mixed(b, d, part):
        return own[b, d, part, :] + precv[b, d, part, :].astype(F32)

    def ring(b, j):
        parts = [slice(0, half), slice(half, Q)]
        if j == 0:
            pair_copy(b, dests[0]).wait_recv()
            for way in range(2):
                hsend[b, way] = mixed(b, dests[0], parts[way]).astype(BF16)
                half_copy(b, way).start()
        elif j == 1:
            for way in range(2):
                d = dests[1 + way]
                pair_copy(b, d).wait_recv()
                half_copy(b, way).wait_recv()
                added = mixed(b, d, parts[way]) + hrecv[b, way].astype(F32)
                fsend[b, way, parts[way], :] = added.astype(BF16)
                fsend[b, way, parts[1 - way], :] = mixed(b, d, parts[1 - way]).astype(BF16)
                full_copy(b, way).start()
        else:
            pair_copy(b, dests[3]).wait_recv()
            full_copy(b, 0).wait_recv()
            full_copy(b, 1).wait_recv()
            at = pl.multiple_of(b * Q, Q)
            base_ref[pl.ds(at, Q), :] = (
                mixed(b, y, slice(0, Q)) + frecv[b, 0].astype(F32) + frecv[b, 1].astype(F32)
            )

    def tick(t, carry):
        @pl.when(t < blocks)
        def _():
            compute(t)

        for j in range(3):
            b = t - LAG[j]

            @pl.when(jnp.logical_and(b >= 0, b < blocks))
            def _():
                ring(b, j)

        return carry

    lax.fori_loop(0, blocks + LAG[2], tick, 0)

    def drain(b, carry):
        for d in range(4):
            pair_copy(b, d).wait_send()
        for way in range(2):
            half_copy(b, way).wait_send()
            full_copy(b, way).wait_send()
        return carry

    lax.fori_loop(0, blocks, drain, 0)


def project(ylg, eg, cc, inc, gain, weight):
    tokens, width = ylg.shape
    feat = weight.shape[1] // 8
    blocks = tokens // Q
    vmem = pl.BlockSpec(memory_space=pltpu.VMEM)
    dma = pltpu.SemaphoreType.DMA
    return pl.pallas_call(
        project_kernel,
        in_specs=[vmem] * 5 + [pl.BlockSpec(memory_space=pl.ANY)],
        out_specs=[vmem, vmem],
        out_shape=[
            jax.ShapeDtypeStruct((tokens, feat), F32),
            jax.ShapeDtypeStruct((tokens, width), BF16),
        ],
        scratch_shapes=[
            pltpu.VMEM((8, width, feat), BF16),
            pltpu.VMEM((blocks, 4, Q, feat), F32),
            pltpu.VMEM((blocks, 4, Q, feat), BF16),
            pltpu.VMEM((blocks, 4, Q, feat), BF16),
            pltpu.VMEM((blocks, 2, Q // 2, feat), BF16),
            pltpu.VMEM((blocks, 2, Q // 2, feat), BF16),
            pltpu.VMEM((blocks, 2, Q, feat), BF16),
            pltpu.VMEM((blocks, 2, Q, feat), BF16),
            dma((8,)), dma((blocks, 4)), dma((blocks, 4)),
            dma((blocks, 2)), dma((blocks, 2)), dma((blocks, 2)), dma((blocks, 2)),
        ],
        compiler_params=pltpu.CompilerParams(
            collective_id=2, has_side_effects=True, vmem_limit_bytes=VMEM_LIMIT
        ),
        name="project",
    )(ylg, eg, cc, inc, gain, weight)


def lowrank_kernel(
    slot_ref, normed_ref, panel_ref, low_ref, lsend, lrecv, lout, sem_ls, sem_lr, sem_as, sem_ar
):
    head = lax.axis_index("head")
    width = normed_ref.shape[1]
    barrier = pltpu.get_barrier_semaphore()
    for k in range(1, 8):
        pl.semaphore_signal(
            barrier, inc=1, device_id={"head": (head + k) % 8}, device_id_type=MESH
        )

    def low_copy(b):
        return pltpu.make_async_remote_copy(
            src_ref=lsend.at[b], dst_ref=lrecv.at[head],
            send_sem=sem_ls.at[b], recv_sem=sem_lr.at[head],
            device_id={"head": b}, device_id_type=MESH,
        )

    def low_arrival(k):
        return pltpu.make_async_remote_copy(
            src_ref=lsend.at[k], dst_ref=lrecv.at[k],
            send_sem=sem_ls.at[k], recv_sem=sem_lr.at[k],
            device_id={"head": k}, device_id_type=MESH,
        )

    def sum_copy(k):
        return pltpu.make_async_remote_copy(
            src_ref=lout.at[head], dst_ref=lout.at[head],
            send_sem=sem_as.at[k], recv_sem=sem_ar.at[head],
            device_id={"head": k}, device_id_type=MESH,
        )

    def sum_arrival(k):
        return pltpu.make_async_remote_copy(
            src_ref=lout.at[k], dst_ref=lout.at[k],
            send_sem=sem_as.at[k], recv_sem=sem_ar.at[k],
            device_id={"head": k}, device_id_type=MESH,
        )

    pl.semaphore_wait(barrier, 7)
    for b in range(8):
        low = dot_dims(
            panel_ref[slot_ref[b], :, 0:width], normed_ref[b * Q : b * Q + Q, :], 1, 1
        ).astype(BF16)
        lsend[b] = low

        @pl.when(b == head)
        def _():
            lrecv[b] = low

        @pl.when(b != head)
        def _():
            low_copy(b).start()

    for k in range(8):
        @pl.when(k != head)
        def _():
            low_arrival(k).wait_recv()
    total = lrecv[0].astype(F32)
    for k in range(1, 8):
        total = total + lrecv[k].astype(F32)
    lout[head] = total.astype(BF16)
    for k in range(8):
        @pl.when(k != head)
        def _():
            sum_copy(k).start()

    for k in range(8):
        @pl.when(k != head)
        def _():
            sum_arrival(k).wait_recv()
            low_copy(k).wait_send()
            sum_copy(k).wait_send()
    low_ref[...] = lout[...]


def lowrank(slots, normed, panels):
    rank = panels.shape[1]
    vmem = pl.BlockSpec(memory_space=pltpu.VMEM)
    dma = pltpu.SemaphoreType.DMA
    return pl.pallas_call(
        lowrank_kernel,
        in_specs=[pl.BlockSpec(memory_space=pltpu.SMEM), vmem, vmem],
        out_specs=vmem,
        out_shape=jax.ShapeDtypeStruct((8, rank, Q), BF16),
        scratch_shapes=[pltpu.VMEM((8, rank, Q), BF16)] * 3 + [dma((8,))] * 4,
        compiler_params=pltpu.CompilerParams(
            collective_id=3, has_side_effects=True, vmem_limit_bytes=16 * 1024 * 1024
        ),
        name="lowrank",
    )(slots, normed, panels)


SLOTS = TURN_DEV + 1


def lay_out_kernel(tenant_ref, index_ref, down_ref, up_ref, out_ref):
    group, width = out_ref.shape[0], down_ref.shape[2]
    first = PANEL_DEV * lax.axis_index("ctx")
    for k in range(group):
        device = pl.program_id(0) * (group // SLOTS) + k // SLOTS
        turn = jnp.maximum(TURN_DEV * device - 1 + k % SLOTS, 0)
        place = index_ref[tenant_ref[turn]] - first
        here = jnp.logical_and(place >= 0, place < PANEL_DEV)
        at = jnp.clip(place, 0, PANEL_DEV - 1)
        out_ref[k, :, 0:width] = jnp.where(here, down_ref[at], 0)
        out_ref[k, :, width:] = jnp.where(here, up_ref[at], 0)


def lay_out(tenants, index, down, up, devices, group=2 * SLOTS):
    rank, width = down.shape[1:]
    total = width + up.shape[2]
    return pl.pallas_call(
        lay_out_kernel,
        grid_spec=pltpu.PrefetchScalarGridSpec(
            num_scalar_prefetch=2,
            grid=(devices * SLOTS // group,),
            in_specs=[
                pl.BlockSpec(down.shape, lambda i, *s: (0, 0, 0)),
                pl.BlockSpec(up.shape, lambda i, *s: (0, 0, 0)),
            ],
            out_specs=pl.BlockSpec((group, rank, total), lambda i, *s: (i, 0, 0)),
        ),
        out_shape=jax.ShapeDtypeStruct((devices * SLOTS, rank, total), BF16),
        name="lay_out",
    )(tenants, index, down, up)


def adapt_kernel(slot_ref, base_ref, low_ref, up_ref, out_ref):
    out_ref[...] = (base_ref[...] + dot_dims(low_ref[0], up_ref[0], 0, 0)).astype(BF16)


def adapt(slots, base, low, up):
    tokens, feat = base.shape
    rank = low.shape[1]
    return pl.pallas_call(
        adapt_kernel,
        grid_spec=pltpu.PrefetchScalarGridSpec(
            num_scalar_prefetch=1,
            grid=(tokens // Q,),
            in_specs=[
                pl.BlockSpec((Q, feat), lambda i, s: (i, 0)),
                pl.BlockSpec((1, rank, Q), lambda i, s: (i, 0, 0)),
                pl.BlockSpec((1, rank, feat), lambda i, s: (s[i], 0, up.shape[2] // feat - 1)),
            ],
            out_specs=pl.BlockSpec((Q, feat), lambda i, s: (i, 0)),
        ),
        out_shape=jax.ShapeDtypeStruct((tokens, feat), BF16),
        compiler_params=pltpu.CompilerParams(vmem_limit_bytes=16 * 1024 * 1024),
        name="adapt",
    )(slots, base, low, up)


def local(
    input_x_channels,
    input_b_channels,
    input_c_channels,
    input_gate_channels,
    raw_step_sizes,
    log_decay_rate,
    head_skip_coeff,
    x_conv_taps,
    b_conv_taps,
    c_conv_taps,
    gated_norm_gain,
    output_weight,
    adapter_down_panels,
    adapter_up_panels,
    turn_first_token,
    tenant_of_turn,
    tenant_panel_index,
):
    tokens = input_x_channels.shape[0]
    own = lax.axis_index("ctx")
    starts = lax.dynamic_slice_in_dim(turn_first_token, TURN_DEV * own, TURN_DEV, 0)
    firsts = own * tokens + Q * jnp.arange(tokens // Q)
    slots = jnp.sum((firsts[:, None] >= starts[None, :]).astype(jnp.int32), axis=1)

    count = lax.axis_size("ctx")
    offered = lay_out(
        tenant_of_turn, tenant_panel_index,
        adapter_down_panels.transpose(0, 2, 1), adapter_up_panels, count,
    )
    panels = lax.psum_scatter(offered, "ctx", scatter_dimension=0, tiled=True)

    tails = jnp.concatenate(
        [input_x_channels[tokens - 8 :], input_b_channels[tokens - 8 :], input_c_channels[tokens - 8 :]],
        axis=1,
    )
    halo = lax.ppermute(tails, "ctx", [(i, i + 1) for i in range(count - 1)])
    ylg, eg, cc, state, decay = local_scan(
        input_x_channels, input_b_channels, input_c_channels, input_gate_channels, raw_step_sizes,
        log_decay_rate, head_skip_coeff, halo, x_conv_taps, b_conv_taps, c_conv_taps,
    )
    inc = exchange(state, decay)
    base, normed = project(ylg, eg, cc, inc, gated_norm_gain.reshape(1, -1), output_weight)
    panels, normed = lax.optimization_barrier((panels, normed))
    low = lowrank(slots, normed, panels)
    return adapt(slots, base, low, panels)


def solution(mesh):
    in_specs = (
        P("ctx", "head"),
        P("ctx", "head"),
        P("ctx", "head"),
        P("ctx", "head"),
        P("head", "ctx"),
        P("head"),
        P("head"),
        P(None, "head"),
        P(None, "head"),
        P(None, "head"),
        P("head"),
        P("head", None),
        P("ctx", "head", None),
        P("ctx", None, "head"),
        P(),
        P(),
        P(),
    )
    out_specs = P("ctx", "head")
    return jax.shard_map(local, mesh=mesh, in_specs=in_specs, out_specs=out_specs, check_vma=False)
```
